8 devices in a mesh: dp: 1 (over z), ing: 2 (over y), grp: 4 (over x, core).
Axes of the slice: x: 2, y: 2, z: 1, core: 2. Of those that a mesh axis runs over, the one named last changes fastest.
Arguments:
- tokens: bfloat16 [1024, 2048], P(('dp', 'grp', 'ing'))
- expert_ids: int32 [1024, 2, 2], P(('dp', 'grp', 'ing'))
- gate_vals: float32 [1024, 2, 2], P(('dp', 'grp', 'ing'))
- w_one: bfloat16 [32, 2048, 1792], P(('grp', 'ing'))
- w_three: bfloat16 [32, 2048, 1792], P(('grp', 'ing'))
- w_two: bfloat16 [32, 1792, 2048], P(('grp', 'ing'))
Outputs:
- output: bfloat16 [1024, 2048], P(('dp', 'grp', 'ing'))
All inputs are finite; a program needn't handle non-finite values.
Results may differ from the reference program's by a relative error of at most 0.00159.
Values are sent between devices in bfloat16 or wider.
A program may use at most 1 GiB of HBM per device.

```python
import jax
import jax.numpy as jnp
from jax import lax

TOK = 128
D = 2048
FF = 1792
EXPERTS = 32
TOP = 4
TOPG = 2
GRP = 4
ING = 2

DEVS = GRP * ING
ROWS = DEVS * TOK
M_GROUPS = min(TOPG, GRP // 2)
PER_GROUP = TOP // M_GROUPS
EXP_GROUP = EXPERTS // GRP
CAP_GROUP = (TOK * M_GROUPS + GRP - 1) // GRP
CAP_EXP = (CAP_GROUP * PER_GROUP + EXP_GROUP - 1) // EXP_GROUP
EXP_ROWS = DEVS * CAP_EXP


def draw_routing(route_key):
    key_perm, key_off, key_gperm, key_eoff, key_eperm = jax.random.split(route_key, 5)
    dev_ids = jnp.arange(DEVS)[:, None, None]
    tok_order = jax.vmap(lambda sub_key: jax.random.permutation(sub_key, TOK))(jax.random.split(key_perm, DEVS))
    grp_perm = jax.vmap(lambda sub_key: jax.random.permutation(sub_key, GRP))(jax.random.split(key_gperm, DEVS))
    exp_perm = jax.vmap(lambda sub_key: jax.random.permutation(sub_key, EXP_GROUP))(jax.random.split(key_eperm, DEVS * GRP)).reshape(DEVS, GRP, EXP_GROUP)
    grp_off = jax.random.randint(key_off, (DEVS, 1, 1), 0, GRP)
    exp_off = jax.random.randint(key_eoff, (DEVS, GRP), 0, EXP_GROUP)
    order_pos = jnp.arange(TOK)[:, None] * M_GROUPS + jnp.arange(M_GROUPS)[None, :]
    residue = (order_pos[None, :, :] + grp_off) % GRP
    res_count = jnp.sum((residue[..., None] == jnp.arange(GRP)).astype(jnp.int32), axis=2)
    earlier = jnp.cumsum(res_count, axis=1) - res_count
    arrival = jnp.take_along_axis(earlier, residue, axis=2)
    group_id = grp_perm[dev_ids, residue]
    slot_pos = (exp_off[dev_ids, residue][..., None] + arrival[..., None] * PER_GROUP + jnp.arange(PER_GROUP)) % EXP_GROUP
    local_exp = jnp.take_along_axis(exp_perm[dev_ids, residue], slot_pos, axis=3)
    expert = group_id[..., None] * EXP_GROUP + local_exp
    routed = expert[jnp.arange(DEVS)[:, None], tok_order]
    return routed.reshape(ROWS, M_GROUPS, PER_GROUP).astype(jnp.int32)


def setup_inputs(seed: int = 0, part: int = 0) -> dict:
    base_key = jax.random.key(seed)
    part_key = jax.random.fold_in(base_key, part)
    key_tok, key_route, key_gate = jax.random.split(part_key, 3)
    key_one, key_three, key_two = jax.random.split(jax.random.key(seed + 1), 3)
    tokens = jax.random.normal(key_tok, (ROWS, D), jnp.float32).astype(jnp.bfloat16)
    expert_ids = draw_routing(key_route)
    gate_vals = jax.random.uniform(key_gate, (ROWS, M_GROUPS, PER_GROUP), jnp.float32, 0.3, 1.7) / TOP
    w_one = (jax.random.normal(key_one, (EXPERTS, D, FF), jnp.float32) * D ** -0.5).astype(jnp.bfloat16)
    w_three = (jax.random.normal(key_three, (EXPERTS, D, FF), jnp.float32) * D ** -0.5).astype(jnp.bfloat16)
    w_two = (jax.random.normal(key_two, (EXPERTS, FF, D), jnp.float32) * (2.0 * FF ** -0.5)).astype(jnp.bfloat16)
    return {'tokens': tokens, 'expert_ids': expert_ids, 'gate_vals': gate_vals, 'w_one': w_one, 'w_three': w_three, 'w_two': w_two}


def expert_rows(x_rows, w_first, w_third, w_second):
    h_one = jnp.dot(x_rows, w_first, preferred_element_type=jnp.float32)
    h_three = jnp.dot(x_rows, w_third, preferred_element_type=jnp.float32)
    act_bf = (jax.nn.silu(h_one) * h_three).astype(jnp.bfloat16)
    return jnp.dot(act_bf, w_second, preferred_element_type=jnp.float32).astype(jnp.bfloat16)


def reference(tokens, expert_ids, gate_vals, w_one, w_three, w_two):
    flat_ids = expert_ids.reshape(ROWS, TOP)
    flat_gate = gate_vals.reshape(ROWS, TOP)
    slot_ids = jnp.arange(EXP_ROWS)

    def one_expert(grp_acc, packed):
        exp_id, w_first, w_third, w_second = packed
        hit_mask = flat_ids == exp_id
        hit_any = jnp.any(hit_mask, axis=1)
        tok_gate = jnp.sum(jnp.where(hit_mask, flat_gate, 0.0), axis=1)
        row_ids = jnp.nonzero(hit_any, size=EXP_ROWS, fill_value=0)[0]
        row_gate = jnp.where(slot_ids < jnp.sum(hit_any.astype(jnp.int32)), tok_gate[row_ids], 0.0)
        exp_out = expert_rows(tokens[row_ids], w_first, w_third, w_second)
        grp_acc = grp_acc.at[row_ids].add(row_gate[:, None] * exp_out.astype(jnp.float32))
        return grp_acc, None

    def one_group(total_sum, packed):
        grp_acc, _ = lax.scan(one_expert, jnp.zeros((ROWS, D), jnp.float32), packed)
        return total_sum + grp_acc.astype(jnp.bfloat16).astype(jnp.float32), None

    packed_all = (jnp.arange(EXPERTS).reshape(GRP, EXP_GROUP), w_one.reshape(GRP, EXP_GROUP, D, FF), w_three.reshape(GRP, EXP_GROUP, D, FF), w_two.reshape(GRP, EXP_GROUP, FF, D))
    total_sum, _ = lax.scan(one_group, jnp.zeros((ROWS, D), jnp.float32), packed_all)
    return total_sum.astype(jnp.bfloat16)
```

```python
import functools

import jax
import jax.numpy as jnp
from jax import lax
from jax.experimental import pallas as pl
from jax.experimental.pallas import tpu as pltpu
from jax.sharding import PartitionSpec as P

MESH = pl.DeviceIdType.MESH
BF16 = jnp.bfloat16
F32 = jnp.float32
I32 = jnp.int32

TOK = 128
D = 2048
FF = 1792
EL = 4
CAP = 16
FC = 256
NF = FF // FC
NC = 512
N4 = D // NC
NB = 256
N8 = D // NB
NS = 22
CH = 4
CR = TOK // CH

BLOCK = {(1, 0, 0): 0, (1, 1, 0): 1, (1, 0, 1): 2, (1, 1, 1): 3,
         (0, 0, 0): 4, (0, 0, 1): 5, (0, 1, 0): 6, (0, 1, 1): 7}
PEERS = [(dy, dx, dc) for dy in (0, 1) for dx in (0, 1) for dc in (0, 1)][1:]
RET = [(0, 32, 1, 0, 0), (32, 32, 1, 1, 0), (80, 16, 0, 1, 0), (112, 16, 0, 1, 16)]


def kernel(ids_ref, gate_ref, tok_hbm, w1, w3, w2, y_ref,
           ring, T, X, act, E, R, PX, Q, PS, CM, GB, GH, META,
           ws_a, ws_b, tsem, bs, br, ss, sr, ms, mr, es, er, ps, pr):
    g = lax.axis_index('grp')
    y = lax.axis_index('ing')
    x = g // 2
    c = g % 2

    def peer(dy, dx, dc):
        return {'ing': (y + dy) % 2, 'grp': ((x + dx) % 2) * 2 + (c + dc) % 2}

    def remote(src, dst, s, r, to):
        return pltpu.make_async_remote_copy(src_ref=src, dst_ref=dst, send_sem=s, recv_sem=r, device_id=peer(*to), device_id_type=MESH)

    def w13(e, f, slot):
        col = pl.ds(pl.multiple_of(f * FC, FC), FC)
        return (pltpu.make_async_copy(w1.at[e, :, col], ring.at[slot, :, pl.ds(0, FC)], ws_a.at[slot]),
                pltpu.make_async_copy(w3.at[e, :, col], ring.at[slot, :, pl.ds(FC, FC)], ws_b.at[slot]))

    def w2c(e, n, slot):
        return (pltpu.make_async_copy(w2.at[e, :, pl.ds(n * NC, NC)], ring.at[slot, pl.ds(0, FF), :], ws_a.at[slot]),)

    def start(copies):
        for cp in copies:
            cp.start()

    def wait(copies):
        for cp in copies:
            cp.wait()

    own = pltpu.make_async_copy(tok_hbm, T.at[0, pl.ds(0, TOK), :], tsem)
    own.start()
    for e in (0, 1):
        for f in range(NF):
            start(w13(e, f, e * 11 + f))
        for n in range(N4):
            start(w2c(e, n, e * 11 + NF + n))

    META[0] = jnp.concatenate([ids_ref[...].astype(F32), gate_ref[...]], axis=0)

    barrier = pltpu.get_barrier_semaphore()
    for p in PEERS:
        pl.semaphore_signal(barrier, inc=1, device_id=peer(*p), device_id_type=MESH)
    pl.semaphore_wait(barrier, len(PEERS))

    metas = [remote(META.at[0], META.at[(p[0] * 2 + p[1]) * 2 + p[2]], ms.at[i], mr.at[i], p) for i, p in enumerate(PEERS)]
    start(metas)
    own.wait()

    def rows(k):
        return pl.ds(k * CR, CR)

    def rows2(k):
        return pl.ds(TOK + k * CR, CR)

    own_y = [remote(T.at[0, rows(k)], T.at[2, rows(k)], bs.at[0, k], br.at[0, k], (1, 0, 0)) for k in range(CH)]
    own_x = [remote(T.at[0, rows(k)], T.at[1, rows(k)], bs.at[1, k], br.at[1, k], (0, 1, 0)) for k in range(CH)]
    own_s = remote(T.at[0, pl.ds(0, TOK)], T.at[0, pl.ds(TOK, TOK)], ss.at[0], sr.at[0], (0, 0, 1))
    fwd = [remote(T.at[2 if k < CH // 2 else 1, rows(k)], T.at[3, rows(k)], bs.at[2, k], br.at[2, k],
                  (0, 1, 0) if k < CH // 2 else (1, 0, 0)) for k in range(CH)]
    y_s = [remote(T.at[2, rows(k)], T.at[2, rows2(k)], bs.at[3, k], br.at[3, k], (0, 0, 1)) for k in range(CH)]
    x_s = [remote(T.at[1, rows(k)], T.at[1, rows2(k)], bs.at[4, k], br.at[4, k], (0, 0, 1)) for k in range(CH)]
    d_s = [remote(T.at[3, rows(k)], T.at[3, rows2(k)], bs.at[5, k], br.at[5, k], (0, 0, 1)) for k in range(CH)]
    for k in range(CH):
        own_y[k].start()
        own_x[k].start()
    own_s.start()

    for m in metas:
        m.wait_recv()
    sub = lax.broadcasted_iota(I32, (TOK, TOK), 0)
    lane = lax.broadcasted_iota(I32, (TOK, TOK), 1)
    base = ((g * 2 + y) * EL).astype(F32)
    hot_rows = []
    for h in range(8):
        ids_h = META[h][0:4, :]
        for e in range(EL):
            hot_rows.append(jnp.sum(jnp.where(ids_h == base + e, 1.0, 0.0), axis=0, keepdims=True))
    hot = jnp.concatenate(hot_rows, axis=0)
    rank = jnp.dot(hot.astype(BF16), (sub < lane).astype(BF16), preferred_element_type=F32)
    key = jnp.where(hot > 0.0, rank, -1.0)
    slot16 = lax.broadcasted_iota(I32, (CAP, TOK), 0).astype(F32)
    zero16 = jnp.zeros((CAP, TOK), F32)
    for q in range(4):
        parts = []
        for e in range(EL):
            for dc in range(2):
                r = (q * 2 + dc) * EL + e
                hit = jnp.where(key[r:r + 1, :] == slot16, 1.0, 0.0)
                parts.append(jnp.concatenate([hit, zero16] if dc == 0 else [zero16, hit], axis=1))
        GH[q] = jnp.concatenate(parts, axis=0).astype(BF16)

    lower = (lane < sub).astype(BF16)
    lane_f = lane.astype(F32)
    col256 = lax.broadcasted_iota(I32, (TOK, 256), 1)
    for dx in range(2):
        meta_t = jnp.transpose(jnp.concatenate([META[dx * 2], jnp.zeros((TOK - 8, TOK), F32)], axis=0))
        ids_c = [meta_t[:, k:k + 1] for k in range(4)]
        gate_c = [meta_t[:, 4 + k:5 + k] for k in range(4)]
        hot_t = sum(jnp.where(ids_c[k] == lane_f, 1.0, 0.0) for k in range(4))
        rank_t = jnp.dot(lower, hot_t.astype(BF16), preferred_element_type=F32)
        row_of, dc_of = [], []
        for k in range(4):
            slot = jnp.sum(jnp.where(ids_c[k] == lane_f, rank_t, 0.0), axis=1, keepdims=True).astype(I32)
            idi = ids_c[k].astype(I32)
            dcr = ((idi >> 3) + c) & 1
            dyr = ((idi >> 2) + y) & 1
            row_of.append(dyr * 128 + (idi & 3) * 32 + dx * 16 + slot)
            dc_of.append(jnp.where((idi >> 4) == x, dcr, 2))
        for dc in range(2):
            for u in range(2):
                sel = [dc_of[2 * m + u] == dc for m in range(2)]
                row = jnp.where(sel[0], row_of[u], jnp.where(sel[1], row_of[2 + u], -1))
                gate = jnp.where(sel[0], gate_c[u], jnp.where(sel[1], gate_c[2 + u], 0.0))
                CM[dc, pl.ds((dx * 2 + u) * TOK, TOK), :] = jnp.where(row == col256, 1.0, 0.0).astype(BF16)
                GB[(dc * 2 + dx) * 2 + u] = jnp.broadcast_to(gate, (TOK, TOK))

    def gather(q):
        dy, dx = q // 2, q % 2
        for n in range(N4):
            cols = pl.ds(n * NC, NC)
            got = jnp.dot(GH[q], T[q, :, cols], preferred_element_type=F32).astype(BF16)
            for e in range(EL):
                for dc in range(2):
                    i = (e * 2 + dc) * CAP
                    X[e, pl.ds(BLOCK[(dy, dx, dc)] * CAP, CAP), cols] = got[i:i + CAP, :]

    for k in range(CH):
        own_y[k].wait_recv()
        y_s[k].start()
        if k < CH // 2:
            fwd[k].start()
        own_x[k].wait_recv()
        x_s[k].start()
        if k >= CH // 2:
            fwd[k].start()
    own_s.wait_recv()
    gather(0)
    for k in range(CH):
        y_s[k].wait_recv()
        x_s[k].wait_recv()
    gather(1)
    gather(2)
    for k in range(CH):
        fwd[k].wait_recv()
        d_s[k].start()
    for k in range(CH):
        d_s[k].wait_recv()
    gather(3)

    def layer1(e, a, f_lo, f_hi, base_slot, after):
        def body(f, carry):
            slot = base_slot + f
            wait(w13(e, f, slot))
            h = jnp.dot(X[e], ring[slot], preferred_element_type=F32)
            h1 = h[:, :FC]
            act[a, :, pl.ds(pl.multiple_of(f * FC, FC), FC)] = (jax.nn.silu(h1) * h[:, FC:]).astype(BF16)
            if after is not None:
                after(f)
            return carry
        lax.fori_loop(f_lo, f_hi, body, 0)

    def layer2(e, a, n, slot):
        wait(w2c(e, n, slot))
        out = jnp.dot(act[a], ring[slot, pl.ds(0, FF), :], preferred_element_type=F32).astype(BF16)
        for i in range(2):
            blk = out[:, i * NB:(i + 1) * NB]
            E[2 * n + i, e] = blk
            R[2 * n + i, 0, 0, e, pl.ds(0, CAP), :] = blk[64:80, :]
            R[2 * n + i, 0, 0, e, pl.ds(CAP, CAP), :] = blk[96:112, :]

    sends = []

    def send(n0, nn, e0, ne, grp):
        for i, (r0, nr, dy, dc, d0) in enumerate(RET):
            cp = remote(E.at[pl.ds(n0, nn), pl.ds(e0, ne), pl.ds(r0, nr), :],
                        R.at[pl.ds(n0, nn), dc, dy, pl.ds(e0, ne), pl.ds(d0, nr), :],
                        es.at[i, grp], er.at[i, grp], (dy, 0, dc))
            cp.start()
            sends.append(cp)

    layer1(0, 0, 0, NF, 0, lambda f: start(w13(2, f, f)))
    for n in range(N4):
        layer2(0, 0, n, NF + n)
        start(w13(3, n, NF + n))
        if n % 2 == 1:
            send(2 * n - 2, 4, 0, 1, n // 2)
    layer1(1, 0, 0, 3, 11, lambda f: start(w13(3, f + 4, 11 + f)))
    for f in range(3, NF):
        layer1(1, 0, f, f + 1, 11, None)
        start(w2c(2 + (f - 3) % 2, (f - 3) // 2, 11 + f))
    for n in range(N4):
        layer2(1, 0, n, 18 + n)
        start(w2c(2 + n % 2, 2 + n // 2, 18 + n))
        if n % 2 == 1:
            send(2 * n - 2, 4, 1, 1, 2 + n // 2)
    layer1(2, 0, 0, NF, 0, None)
    layer1(3, 1, 0, NF, 7, None)
    for n in range(N4):
        for e in (2, 3):
            layer2(e, e - 2, n, 14 + 2 * n + e - 2)
        for i in range(2):
            send(2 * n + i, 1, 2, 2, 4 + 2 * n + i)

    gone = [remote(PX.at[n], Q.at[n], ps.at[n], pr.at[n], (0, 1, 0)) for n in range(N8)]

    def finish(n):
        gone[n].wait_recv()
        y_ref[:, pl.ds(n * NB, NB)] = (PS[n].astype(F32) + Q[n].astype(F32)).astype(BF16)

    for n in range(N8):
        if n % 4 == 0:
            for cp in sends[4 * (n // 4):4 * (n // 4) + 4] + sends[8 + 4 * (n // 4):8 + 4 * (n // 4) + 4]:
                cp.wait_recv()
        for cp in sends[16 + 4 * n:16 + 4 * n + 4]:
            cp.wait_recv()
        rows_n = [R[n, dc].reshape(256, NB) for dc in range(2)]
        for dx in (1, 0):
            total = jnp.zeros((TOK, NB), F32)
            for dc in range(2):
                part = jnp.dot(CM[dc, pl.ds(dx * 2 * TOK, 2 * TOK), :], rows_n[dc], preferred_element_type=F32)
                g0 = GB[(dc * 2 + dx) * 2]
                g1 = GB[(dc * 2 + dx) * 2 + 1]
                g0 = jnp.concatenate([g0, g0], axis=1)
                g1 = jnp.concatenate([g1, g1], axis=1)
                total = total + (g0 * part[:TOK] + g1 * part[TOK:]).astype(BF16).astype(F32)
            if dx == 1:
                PX[n] = total.astype(BF16)
                gone[n].start()
            else:
                PS[n] = total.astype(BF16)
        if n >= 2:
            finish(n - 2)
    finish(N8 - 2)
    finish(N8 - 1)

    for cp in metas + own_y + own_x + [own_s] + fwd + y_s + x_s + d_s + sends + gone:
        cp.wait_send()


def solution(mesh):
    row_spec = P(('dp', 'grp', 'ing'))
    exp_spec = P(('grp', 'ing'))

    def local_fn(tokens, expert_ids, gate_vals, w_one, w_three, w_two):
        ids = expert_ids.reshape(TOK, 4).T
        gates = gate_vals.reshape(TOK, 4).T
        dma = pltpu.SemaphoreType.DMA
        anywhere = pl.BlockSpec(memory_space=pl.ANY)
        vmem = pl.BlockSpec(memory_space=pltpu.VMEM)
        return pl.pallas_call(
            kernel,
            out_shape=jax.ShapeDtypeStruct((TOK, D), BF16),
            in_specs=[vmem, vmem, anywhere, anywhere, anywhere, anywhere],
            out_specs=vmem,
            scratch_shapes=[
                pltpu.VMEM((NS, D, 2 * FC), BF16),
                pltpu.VMEM((4, 2 * TOK, D), BF16),
                pltpu.VMEM((EL, 8 * CAP, D), BF16),
                pltpu.VMEM((2, 8 * CAP, FF), BF16),
                pltpu.VMEM((N8, EL, 8 * CAP, NB), BF16),
                pltpu.VMEM((N8, 2, 2, EL, 2 * CAP, NB), BF16),
                pltpu.VMEM((N8, TOK, NB), BF16),
                pltpu.VMEM((N8, TOK, NB), BF16),
                pltpu.VMEM((N8, TOK, NB), BF16),
                pltpu.VMEM((2, 4 * TOK, 256), BF16),
                pltpu.VMEM((8, TOK, TOK), F32),
                pltpu.VMEM((4, 128, 256), BF16),
                pltpu.VMEM((8, 8, TOK), F32),
                dma((NS,)), dma((NS,)), dma(()),
                dma((6, CH)), dma((6, CH)), dma((1,)), dma((1,)),
                dma((7,)), dma((7,)),
                dma((4, 12)), dma((4, 12)), dma((N8,)), dma((N8,)),
            ],
            compiler_params=pltpu.CompilerParams(collective_id=0, has_side_effects=True, vmem_limit_bytes=67043328),
        )(ids, gates, tokens, w_one, w_three, w_two)

    return jax.shard_map(local_fn, mesh=mesh, in_specs=(row_spec, row_spec, row_spec, exp_spec, exp_spec, exp_spec), out_specs=row_spec, check_vma=False)
```

```python
import functools

import jax
import jax.numpy as jnp
from jax import lax
from jax.experimental import pallas as pl
from jax.experimental.pallas import tpu as pltpu
from jax.sharding import PartitionSpec as P

MESH = pl.DeviceIdType.MESH
BF16 = jnp.bfloat16
F32 = jnp.float32
I32 = jnp.int32

TOK = 128
D = 2048
FF = 1792
EL = 4
CAP = 16
FC = 256
NF = FF // FC
NC = 512
N4 = D // NC
NB = 256
N8 = D // NB
NS = 22
CH = 4
CR = TOK // CH

BLOCK = {(1, 0, 0): 0, (1, 1, 0): 1, (1, 0, 1): 2, (1, 1, 1): 3,
         (0, 0, 0): 4, (0, 0, 1): 5, (0, 1, 0): 6, (0, 1, 1): 7}
PEERS = [(dy, dx, dc) for dy in (0, 1) for dx in (0, 1) for dc in (0, 1)][1:]
RET = [(0, 32, 1, 0, 0), (32, 32, 1, 1, 0), (80, 16, 0, 1, 0), (112, 16, 0, 1, 16)]


def kernel(ids_ref, gate_ref, tok_hbm, w1, w3, w2, y_ref,
           ring, T, X, act, E, R, PX, Q, PS, CM, GB, GH, META,
           ws_a, ws_b, tsem, bs, br, ss, sr, ms, mr, es, er, ps, pr):
    g = lax.axis_index('grp')
    y = lax.axis_index('ing')
    x = g // 2
    c = g % 2

    def peer(dy, dx, dc):
        return {'ing': (y + dy) % 2, 'grp': ((x + dx) % 2) * 2 + (c + dc) % 2}

    def remote(src, dst, s, r, to):
        return pltpu.make_async_remote_copy(src_ref=src, dst_ref=dst, send_sem=s, recv_sem=r, device_id=peer(*to), device_id_type=MESH)

    def w13(e, f, slot):
        col = pl.ds(pl.multiple_of(f * FC, FC), FC)
        return (pltpu.make_async_copy(w1.at[e, :, col], ring.at[slot, :, pl.ds(0, FC)], ws_a.at[slot]),
                pltpu.make_async_copy(w3.at[e, :, col], ring.at[slot, :, pl.ds(FC, FC)], ws_b.at[slot]))

    def w2c(e, n, slot):
        return (pltpu.make_async_copy(w2.at[e, :, pl.ds(n * NC, NC)], ring.at[slot, pl.ds(0, FF), :], ws_a.at[slot]),)

    def start(copies):
        for cp in copies:
            cp.start(priority=1)

    def wait(copies):
        for cp in copies:
            cp.wait()

    own = pltpu.make_async_copy(tok_hbm, T.at[0, pl.ds(0, TOK), :], tsem)
    own.start()
    for e in (0, 1):
        for f in range(NF):
            start(w13(e, f, e * 11 + f))
        for n in range(N4):
            start(w2c(e, n, e * 11 + NF + n))

    META[0] = jnp.concatenate([ids_ref[...].astype(F32), gate_ref[...]], axis=0)

    barrier = pltpu.get_barrier_semaphore()
    for p in PEERS:
        pl.semaphore_signal(barrier, inc=1, device_id=peer(*p), device_id_type=MESH)
    pl.semaphore_wait(barrier, len(PEERS))

    metas = [remote(META.at[0], META.at[(p[0] * 2 + p[1]) * 2 + p[2]], ms.at[i], mr.at[i], p) for i, p in enumerate(PEERS)]
    for cp in metas:
        cp.start()
    own.wait()

    def rows(k):
        return pl.ds(k * CR, CR)

    def rows2(k):
        return pl.ds(TOK + k * CR, CR)

    own_y = [remote(T.at[0, rows(k)], T.at[2, rows(k)], bs.at[0, k], br.at[0, k], (1, 0, 0)) for k in range(CH)]
    own_x = [remote(T.at[0, rows(k)], T.at[1, rows(k)], bs.at[1, k], br.at[1, k], (0, 1, 0)) for k in range(CH)]
    own_s = remote(T.at[0, pl.ds(0, TOK)], T.at[0, pl.ds(TOK, TOK)], ss.at[0], sr.at[0], (0, 0, 1))
    fwd = [remote(T.at[2 if k < CH // 2 else 1, rows(k)], T.at[3, rows(k)], bs.at[2, k], br.at[2, k],
                  (0, 1, 0) if k < CH // 2 else (1, 0, 0)) for k in range(CH)]
    y_s = [remote(T.at[2, rows(k)], T.at[2, rows2(k)], bs.at[3, k], br.at[3, k], (0, 0, 1)) for k in range(CH)]
    x_s = [remote(T.at[1, rows(k)], T.at[1, rows2(k)], bs.at[4, k], br.at[4, k], (0, 0, 1)) for k in range(CH)]
    d_s = [remote(T.at[3, rows(k)], T.at[3, rows2(k)], bs.at[5, k], br.at[5, k], (0, 0, 1)) for k in range(CH)]
    for k in range(CH):
        own_y[k].start()
        own_x[k].start()
    own_s.start()

    for m in metas:
        m.wait_recv()
    sub = lax.broadcasted_iota(I32, (TOK, TOK), 0)
    lane = lax.broadcasted_iota(I32, (TOK, TOK), 1)
    base = ((g * 2 + y) * EL).astype(F32)
    hot_rows = []
    for h in range(8):
        ids_h = META[h][0:4, :]
        for e in range(EL):
            hot_rows.append(jnp.sum(jnp.where(ids_h == base + e, 1.0, 0.0), axis=0, keepdims=True))
    hot = jnp.concatenate(hot_rows, axis=0)
    rank = jnp.dot(hot.astype(BF16), (sub < lane).astype(BF16), preferred_element_type=F32)
    key = jnp.where(hot > 0.0, rank, -1.0)
    slot16 = lax.broadcasted_iota(I32, (CAP, TOK), 0).astype(F32)
    zero16 = jnp.zeros((CAP, TOK), F32)
    for q in range(4):
        parts = []
        for e in range(EL):
            for dc in range(2):
                r = (q * 2 + dc) * EL + e
                hit = jnp.where(key[r:r + 1, :] == slot16, 1.0, 0.0)
                parts.append(jnp.concatenate([hit, zero16] if dc == 0 else [zero16, hit], axis=1))
        GH[q] = jnp.concatenate(parts, axis=0).astype(BF16)

    lower = (lane < sub).astype(BF16)
    lane_f = lane.astype(F32)
    col256 = lax.broadcasted_iota(I32, (TOK, 256), 1)
    for dx in range(2):
        meta_t = jnp.transpose(jnp.concatenate([META[dx * 2], jnp.zeros((TOK - 8, TOK), F32)], axis=0))
        ids_c = [meta_t[:, k:k + 1] for k in range(4)]
        gate_c = [meta_t[:, 4 + k:5 + k] for k in range(4)]
        hot_t = sum(jnp.where(ids_c[k] == lane_f, 1.0, 0.0) for k in range(4))
        rank_t = jnp.dot(lower, hot_t.astype(BF16), preferred_element_type=F32)
        row_of, dc_of = [], []
        for k in range(4):
            slot = jnp.sum(jnp.where(ids_c[k] == lane_f, rank_t, 0.0), axis=1, keepdims=True).astype(I32)
            idi = ids_c[k].astype(I32)
            dcr = ((idi >> 3) + c) & 1
            dyr = ((idi >> 2) + y) & 1
            row_of.append(dyr * 128 + (idi & 3) * 32 + dx * 16 + slot)
            dc_of.append(jnp.where((idi >> 4) == x, dcr, 2))
        for dc in range(2):
            for u in range(2):
                sel = [dc_of[2 * m + u] == dc for m in range(2)]
                row = jnp.where(sel[0], row_of[u], jnp.where(sel[1], row_of[2 + u], -1))
                gate = jnp.where(sel[0], gate_c[u], jnp.where(sel[1], gate_c[2 + u], 0.0))
                CM[dc, pl.ds((dx * 2 + u) * TOK, TOK), :] = jnp.where(row == col256, 1.0, 0.0).astype(BF16)
                GB[(dc * 2 + dx) * 2 + u] = jnp.broadcast_to(gate, (TOK, TOK))

    def gather(q):
        dy, dx = q // 2, q % 2
        for n in range(N4):
            cols = pl.ds(n * NC, NC)
            got = jnp.dot(GH[q], T[q, :, cols], preferred_element_type=F32).astype(BF16)
            for e in range(EL):
                for dc in range(2):
                    i = (e * 2 + dc) * CAP
                    X[e, pl.ds(BLOCK[(dy, dx, dc)] * CAP, CAP), cols] = got[i:i + CAP, :]

    for k in range(CH):
        own_y[k].wait_recv()
        y_s[k].start()
        if k < CH // 2:
            fwd[k].start()
        own_x[k].wait_recv()
        x_s[k].start()
        if k >= CH // 2:
            fwd[k].start()
    own_s.wait_recv()
    gather(0)
    for k in range(CH):
        y_s[k].wait_recv()
        x_s[k].wait_recv()
    gather(1)
    gather(2)
    for k in range(CH):
        fwd[k].wait_recv()
        d_s[k].start()
    for k in range(CH):
        d_s[k].wait_recv()
    gather(3)

    def layer1(e, a, f, slot):
        wait(w13(e, f, slot))
        h = jnp.dot(X[e], ring[slot], preferred_element_type=F32)
        h1 = h[:, :FC]
        act[a, :, pl.ds(f * FC, FC)] = (jax.nn.silu(h1) * h[:, FC:]).astype(BF16)

    def layer2(e, a, n, slot):
        wait(w2c(e, n, slot))
        out = jnp.dot(act[a], ring[slot, pl.ds(0, FF), :], preferred_element_type=F32).astype(BF16)
        for i in range(2):
            blk = out[:, i * NB:(i + 1) * NB]
            E[2 * n + i, e] = blk
            R[2 * n + i, 0, 0, e, pl.ds(0, CAP), :] = blk[64:80, :]
            R[2 * n + i, 0, 0, e, pl.ds(CAP, CAP), :] = blk[96:112, :]

    sends = []
    arrive = {}

    def send(n0, nn, e0, ne, grp):
        for i, (r0, nr, dy, dc, d0) in enumerate(RET):
            cp = remote(E.at[pl.ds(n0, nn), pl.ds(e0, ne), pl.ds(r0, nr), :],
                        R.at[pl.ds(n0, nn), dc, dy, pl.ds(e0, ne), pl.ds(d0, nr), :],
                        es.at[i, grp], er.at[i, grp], (dy, 0, dc))
            cp.start()
            sends.append(cp)
            arrive.setdefault(grp, []).append(cp)

    for f in range(NF):
        layer1(0, 0, f, f)
        start(w13(2, f, f))
    for n in range(N4):
        layer2(0, 0, n, NF + n)
        start(w13(3, n, NF + n))
        send(2 * n, 2, 0, 1, n)
    for f in range(NF):
        layer1(1, 1, f, 11 + f)
        if f < 3:
            start(w13(3, f + 4, 11 + f))
        else:
            start(w2c(2 + (f - 3) % 2, (f - 3) // 2, 11 + f))
    for n in range(N4):
        layer2(1, 1, n, 18 + n)
        start(w2c(2 + n % 2, 2 + n // 2, 18 + n))
        send(2 * n, 2, 1, 1, 4 + n)
    for e in (2, 3):
        for f in range(NF):
            layer1(e, e - 2, f, (e - 2) * NF + f)
    for n in range(N4):
        for e in (2, 3):
            layer2(e, e - 2, n, 14 + 2 * n + e - 2)
        for i in range(2):
            send(2 * n + i, 1, 2, 2, 8 + 2 * n + i)

    gone = [remote(PX.at[n], Q.at[n], ps.at[n], pr.at[n], (0, 1, 0)) for n in range(N8)]

    def finish(n):
        gone[n].wait_recv()
        y_ref[:, pl.ds(n * NB, NB)] = (PS[n].astype(F32) + Q[n].astype(F32)).astype(BF16)

    for n in range(N8):
        for grp in ([n // 2, 4 + n // 2] if n % 2 == 0 else []) + [8 + n]:
            for cp in arrive[grp]:
                cp.wait_recv()
        rows_n = [R[n, dc].reshape(256, NB) for dc in range(2)]
        for dx in (1, 0):
            total = jnp.zeros((TOK, NB), F32)
            for dc in range(2):
                part = jnp.dot(CM[dc, pl.ds(dx * 2 * TOK, 2 * TOK), :], rows_n[dc], preferred_element_type=F32)
                g0 = GB[(dc * 2 + dx) * 2]
                g1 = GB[(dc * 2 + dx) * 2 + 1]
                g0 = jnp.concatenate([g0, g0], axis=1)
                g1 = jnp.concatenate([g1, g1], axis=1)
                total = total + (g0 * part[:TOK] + g1 * part[TOK:]).astype(BF16).astype(F32)
            if dx == 1:
                PX[n] = total.astype(BF16)
                gone[n].start()
            else:
                PS[n] = total.astype(BF16)
        if n >= 2:
            finish(n - 2)
    finish(N8 - 2)
    finish(N8 - 1)

    for cp in metas + own_y + own_x + [own_s] + fwd + y_s + x_s + d_s + sends + gone:
        cp.wait_send()


def solution(mesh):
    row_spec = P(('dp', 'grp', 'ing'))
    exp_spec = P(('grp', 'ing'))

    def local_fn(tokens, expert_ids, gate_vals, w_one, w_three, w_two):
        ids = expert_ids.reshape(TOK, 4).T
        gates = gate_vals.reshape(TOK, 4).T
        dma = pltpu.SemaphoreType.DMA
        anywhere = pl.BlockSpec(memory_space=pl.ANY)
        vmem = pl.BlockSpec(memory_space=pltpu.VMEM)
        return pl.pallas_call(
            kernel,
            out_shape=jax.ShapeDtypeStruct((TOK, D), BF16),
            in_specs=[vmem, vmem, anywhere, anywhere, anywhere, anywhere],
            out_specs=vmem,
            scratch_shapes=[
                pltpu.VMEM((NS, D, 2 * FC), BF16),
                pltpu.VMEM((4, 2 * TOK, D), BF16),
                pltpu.VMEM((EL, 8 * CAP, D), BF16),
                pltpu.VMEM((2, 8 * CAP, FF), BF16),
                pltpu.VMEM((N8, EL, 8 * CAP, NB), BF16),
                pltpu.VMEM((N8, 2, 2, EL, 2 * CAP, NB), BF16),
                pltpu.VMEM((N8, TOK, NB), BF16),
                pltpu.VMEM((N8, TOK, NB), BF16),
                pltpu.VMEM((N8, TOK, NB), BF16),
                pltpu.VMEM((2, 4 * TOK, 256), BF16),
                pltpu.VMEM((8, TOK, TOK), F32),
                pltpu.VMEM((4, 128, 256), BF16),
                pltpu.VMEM((8, 8, TOK), F32),
                dma((NS,)), dma((NS,)), dma(()),
                dma((6, CH)), dma((6, CH)), dma((1,)), dma((1,)),
                dma((7,)), dma((7,)),
                dma((4, 16)), dma((4, 16)), dma((N8,)), dma((N8,)),
            ],
            compiler_params=pltpu.CompilerParams(collective_id=0, has_side_effects=True, vmem_limit_bytes=67043328),
        )(ids, gates, tokens, w_one, w_three, w_two)

    return jax.shard_map(local_fn, mesh=mesh, in_specs=(row_spec, row_spec, row_spec, exp_spec, exp_spec, exp_spec), out_specs=row_spec, check_vma=False)
```

```python
import functools

import jax
import jax.numpy as jnp
from jax import lax
from jax.experimental import pallas as pl
from jax.experimental.pallas import tpu as pltpu
from jax.sharding import PartitionSpec as P

MESH = pl.DeviceIdType.MESH
BF16 = jnp.bfloat16
F32 = jnp.float32
I32 = jnp.int32

TOK = 128
D = 2048
FF = 1792
EL = 4
CAP = 16
FC = 256
NF = FF // FC
NC = 512
N4 = D // NC
NB = 256
N8 = D // NB
CH = 4
CR = TOK // CH

NS = 24

BLOCK = {(1, 0, 0): 0, (1, 0, 1): 1, (0, 0, 0): 2, (0, 0, 1): 3,
         (0, 1, 0): 4, (0, 1, 1): 5, (1, 1, 0): 6, (1, 1, 1): 7}
NEAR = 6 * CAP
PEERS = [(dy, dx, dc) for dy in (0, 1) for dx in (0, 1) for dc in (0, 1)][1:]
RET = [(0, 1, 0, 0), (16, 1, 1, 0), (48, 0, 1, 0), (80, 0, 1, 16), (96, 1, 0, 16), (112, 1, 1, 16)]

FETCH = []
for _e in (1, 0):
    FETCH += [(1, _e, _f) for _f in range(NF)] + [(2, _e, _n) for _n in range(N4)]
for _e in (2, 3):
    FETCH += [(1, _e, _f) for _f in range(NF)]
for _n in range(N4):
    FETCH += [(2, _e, _n) for _e in (2, 3)]
ACT = {1: 0, 2: 1, 3: 2, 0: 2}


def kernel(ids_ref, gate_ref, tok_hbm, w1, w3, w2, y_hbm,
           ring, T, X, act, E, R, PX, Q, PS, CM, GB, GH, META,
           ws_a, ws_b, tsem, bs, br, ss, sr, ms, mr, es, er, ps, pr, ysem):
    g = lax.axis_index('grp')
    y = lax.axis_index('ing')
    x = g // 2
    c = g % 2

    def peer(dy, dx, dc):
        return {'ing': (y + dy) % 2, 'grp': ((x + dx) % 2) * 2 + (c + dc) % 2}

    def remote(src, dst, s, r, to):
        return pltpu.make_async_remote_copy(src_ref=src, dst_ref=dst, send_sem=s, recv_sem=r, device_id=peer(*to), device_id_type=MESH)

    def w13(e, f, slot):
        col = pl.ds(pl.multiple_of(f * FC, FC), FC)
        return (pltpu.make_async_copy(w1.at[e, :, col], ring.at[slot, :, pl.ds(0, FC)], ws_a.at[slot]),
                pltpu.make_async_copy(w3.at[e, :, col], ring.at[slot, :, pl.ds(FC, FC)], ws_b.at[slot]))

    def w2c(e, n, slot):
        return (pltpu.make_async_copy(w2.at[e, :, pl.ds(n * NC, NC)], ring.at[slot, pl.ds(0, FF), :], ws_a.at[slot]),)

    def start(copies):
        for cp in copies:
            cp.start(priority=1)

    def wait(copies):
        for cp in copies:
            cp.wait()

    own = pltpu.make_async_copy(tok_hbm, T.at[0, pl.ds(0, TOK), :], tsem)
    own.start()
    slot_of = {}
    queue = list(FETCH)

    def fetch(chunk):
        layer, e, j = chunk
        return (w13 if layer == 1 else w2c)(e, j, slot_of[chunk])

    def refill(slot):
        if queue:
            chunk = queue.pop(0)
            slot_of[chunk] = slot
            start(fetch(chunk))

    for i in range(NS):
        refill(i)

    META[0] = jnp.concatenate([ids_ref[...].astype(F32), gate_ref[...]], axis=0)

    barrier = pltpu.get_barrier_semaphore()
    direct = [(0, 0, 1), (0, 1, 0), (1, 0, 0), (1, 0, 1)]
    for p in direct:
        pl.semaphore_signal(barrier, inc=1, device_id=peer(*p), device_id_type=MESH)
    pl.semaphore_wait(barrier, len(direct))

    metas = [remote(META.at[i], META.at[j], ms.at[k], mr.at[k], to) for k, (i, j, to) in enumerate([
        (0, 4, (1, 0, 0)), (0, 2, (0, 1, 0)), (0, 1, (0, 0, 1)),
        (4, 5, (0, 0, 1)), (4, 6, (0, 1, 0)), (2, 3, (0, 0, 1)), (6, 7, (0, 0, 1))])]
    for m in metas[:3]:
        m.start()
    own.wait()

    def rows(k):
        return pl.ds(k * CR, CR)

    def rows2(k):
        return pl.ds(TOK + k * CR, CR)

    own_y = [remote(T.at[0, rows(k)], T.at[2, rows(k)], bs.at[0, k], br.at[0, k], (1, 0, 0)) for k in range(CH)]
    own_x = [remote(T.at[0, rows(k)], T.at[1, rows(k)], bs.at[1, k], br.at[1, k], (0, 1, 0)) for k in range(CH)]
    own_s = remote(T.at[0, pl.ds(0, TOK)], T.at[0, pl.ds(TOK, TOK)], ss.at[0], sr.at[0], (0, 0, 1))
    fwd = [remote(T.at[2 if k < CH // 2 else 1, rows(k)], T.at[3, rows(k)], bs.at[2, k], br.at[2, k],
                  (0, 1, 0) if k < CH // 2 else (1, 0, 0)) for k in range(CH)]
    y_s = [remote(T.at[2, rows(k)], T.at[2, rows2(k)], bs.at[3, k], br.at[3, k], (0, 0, 1)) for k in range(CH)]
    x_s = [remote(T.at[1, rows(k)], T.at[1, rows2(k)], bs.at[4, k], br.at[4, k], (0, 0, 1)) for k in range(CH)]
    d_s = [remote(T.at[3, rows(k)], T.at[3, rows2(k)], bs.at[5, k], br.at[5, k], (0, 0, 1)) for k in range(CH)]
    own_y[0].start()
    own_x[0].start()
    metas[0].wait_recv()
    metas[4].start()
    metas[3].start()
    metas[1].wait_recv()
    metas[5].start()
    for k in range(1, CH):
        own_y[k].start()
        own_x[k].start()
    own_s.start()

    metas[4].wait_recv()
    metas[6].start()
    for i in (2, 3, 5, 6):
        metas[i].wait_recv()
    sub = lax.broadcasted_iota(I32, (TOK, TOK), 0)
    lane = lax.broadcasted_iota(I32, (TOK, TOK), 1)
    base = ((g * 2 + y) * EL).astype(F32)
    hot_rows = []
    for h in range(8):
        ids_h = META[h][0:4, :]
        for e in range(EL):
            hot_rows.append(jnp.sum(jnp.where(ids_h == base + e, 1.0, 0.0), axis=0, keepdims=True))
    hot = jnp.concatenate(hot_rows, axis=0)
    rank = jnp.dot(hot.astype(BF16), (sub < lane).astype(BF16), preferred_element_type=F32)
    key = jnp.where(hot > 0.0, rank, -1.0)
    slot16 = lax.broadcasted_iota(I32, (CAP, TOK), 0).astype(F32)
    zero16 = jnp.zeros((CAP, TOK), F32)
    for q in range(4):
        parts = []
        for e in range(EL):
            for dc in range(2):
                r = (q * 2 + dc) * EL + e
                hit = jnp.where(key[r:r + 1, :] == slot16, 1.0, 0.0)
                parts.append(jnp.concatenate([hit, zero16] if dc == 0 else [zero16, hit], axis=1))
        GH[q] = jnp.concatenate(parts, axis=0).astype(BF16)

    lower = (lane < sub).astype(BF16)
    lane_f = lane.astype(F32)
    for dx in range(2):
        meta_t = jnp.transpose(jnp.concatenate([META[dx * 2], jnp.zeros((TOK - 8, TOK), F32)], axis=0))
        ids_c = [meta_t[:, k:k + 1] for k in range(4)]
        gate_c = [meta_t[:, 4 + k:5 + k] for k in range(4)]
        hot_t = sum(jnp.where(ids_c[k] == lane_f, 1.0, 0.0) for k in range(4))
        rank_t = jnp.dot(lower, hot_t.astype(BF16), preferred_element_type=F32)
        row_of, dc_of = [], []
        for k in range(4):
            slot = jnp.sum(jnp.where(ids_c[k] == lane_f, rank_t, 0.0), axis=1, keepdims=True).astype(I32)
            idi = ids_c[k].astype(I32)
            dcr = ((idi >> 3) + c) & 1
            dyr = ((idi >> 2) + y) & 1
            row_of.append(dyr * 64 + (idi & 3) * CAP + slot)
            dc_of.append(jnp.where((idi >> 4) == x, dcr, 2))
        for dc in range(2):
            for u in range(2):
                sel = [dc_of[2 * m + u] == dc for m in range(2)]
                row = jnp.where(sel[0], row_of[u], jnp.where(sel[1], row_of[2 + u], -1))
                gate = jnp.where(sel[0], gate_c[u], jnp.where(sel[1], gate_c[2 + u], 0.0))
                CM[dc, pl.ds((dx * 2 + u) * TOK, TOK), :] = jnp.where(row == lane, 1.0, 0.0).astype(BF16)
                GB[(dc * 2 + dx) * 2 + u] = jnp.broadcast_to(gate, (TOK, TOK))

    def gather(q):
        dy, dx = q // 2, q % 2
        for n in range(N4):
            cols = pl.ds(n * NC, NC)
            got = jnp.dot(GH[q], T[q, :, cols], preferred_element_type=F32).astype(BF16)
            for e in range(EL):
                for dc in range(2):
                    i = (e * 2 + dc) * CAP
                    X[e, pl.ds(BLOCK[(dy, dx, dc)] * CAP, CAP), cols] = got[i:i + CAP, :]

    def far(k):
        fwd[k].wait_recv()
        d_s[k].start()

    for k in range(CH):
        own_y[k].wait_recv()
        y_s[k].start()
        if k < CH // 2:
            fwd[k].start()
        own_x[k].wait_recv()
        x_s[k].start()
        if k >= CH // 2:
            fwd[k].start()
    own_s.wait_recv()
    gather(0)
    for k in range(CH):
        y_s[k].wait_recv()
        x_s[k].wait_recv()
    gather(1)
    gather(2)

    waited = set()

    def layer1(chunk, r0, r1):
        _, e, f = chunk
        h = jnp.dot(X[e, r0:r1, :], ring[slot_of[chunk]], preferred_element_type=F32)
        h1 = h[:, :FC]
        act[ACT[e], r0:r1, f * FC:(f + 1) * FC] = (jax.nn.silu(h1) * h[:, FC:]).astype(BF16)

    def layer2(chunk, r0, r1):
        _, e, n = chunk
        out = jnp.dot(act[ACT[e], r0:r1, :], ring[slot_of[chunk], 0:FF, :], preferred_element_type=F32).astype(BF16)
        for t in range(2):
            blk = out[:, t * NB:(t + 1) * NB]
            E[2 * n + t, e, r0:r1, :] = blk
            if r0 == 0:
                R[2 * n + t, 0, 0, e, 0:CAP, :] = blk[32:48, :]
                R[2 * n + t, 0, 0, e, CAP:2 * CAP, :] = blk[64:80, :]

    def run(todo, last=True):
        for chunk, _, _ in todo:
            if chunk not in waited:
                waited.add(chunk)
                wait(fetch(chunk))
        for chunk, r0, r1 in todo:
            (layer1 if chunk[0] == 1 else layer2)(chunk, r0, r1)
        if last:
            for chunk, _, _ in todo:
                refill(slot_of[chunk])

    sends = []
    arrive = {(dx, n): [] for dx in range(2) for n in range(N8)}

    def send(parts, n0, nn, e0, ne):
        for i in parts:
            r0, dy, dc, d0 = RET[i]
            k = len(sends)
            cp = remote(E.at[pl.ds(n0, nn), pl.ds(e0, ne), pl.ds(r0, CAP), :],
                        R.at[pl.ds(n0, nn), dc, dy, pl.ds(e0, ne), pl.ds(d0, CAP), :],
                        es.at[k], er.at[k], (dy, 0, dc))
            cp.start()
            sends.append(cp)
            arrive[d0 // CAP, n0].append(cp)

    def l1(e, lo, hi, r0=0, r1=8 * CAP):
        return [((1, e, f), r0, r1) for f in range(lo, hi)]

    def l2(e, lo, hi, r0=0, r1=8 * CAP):
        return [((2, e, n), r0, r1) for n in range(lo, hi)]

    def far(k):
        fwd[k].wait_recv()
        d_s[k].start()

    run(l1(1, 0, NF, 0, NEAR), False)
    far(0)
    far(2)
    run(l2(1, 0, N4, 0, NEAR), False)
    send((0, 1, 2, 3), 0, N8, 1, 1)
    far(1)
    far(3)
    for k in range(CH):
        d_s[k].wait_recv()
    gather(3)
    run(l1(1, 0, 3, NEAR))
    run(l1(1, 3, NF, NEAR) + l1(0, 0, 3))
    run(l1(0, 3, NF))
    for n in (0, 2):
        run(l2(0, n, n + 2))
        send((4, 5, 3, 0, 1, 2), 2 * n, 4, 0, 1)
    for e in (2, 3):
        run(l1(e, 0, 4))
        run(l1(e, 4, NF))
    for n in range(N4):
        run(l2(1, n, n + 1, NEAR) + l2(2, n, n + 1) + l2(3, n, n + 1))
        for t in range(2):
            send((4, 5), 2 * n + t, 1, 1, 3)
            send((3,), 2 * n + t, 1, 2, 2)
    for n in range(N4):
        send((0, 1, 2), 2 * n, 2, 2, 2)

    gone = [remote(PX.at[n], Q.at[n], ps.at[n], pr.at[n], (0, 1, 0)) for n in range(N8)]

    outs = [pltpu.make_async_copy(PS.at[n], y_hbm.at[:, pl.ds(n * NB, NB)], ysem.at[n]) for n in range(N8)]

    def combine(dx, n):
        for cp in arrive[dx, n]:
            cp.wait_recv()
        total = jnp.zeros((TOK, NB), F32)
        for dc in range(2):
            part = jnp.dot(CM[dc, pl.ds(dx * 2 * TOK, 2 * TOK), :], R[n, dc, :, :, pl.ds(dx * CAP, CAP), :].reshape(128, NB), preferred_element_type=F32)
            g0 = GB[(dc * 2 + dx) * 2]
            g1 = GB[(dc * 2 + dx) * 2 + 1]
            g0 = jnp.concatenate([g0, g0], axis=1)
            g1 = jnp.concatenate([g1, g1], axis=1)
            total = total + (g0 * part[:TOK] + g1 * part[TOK:]).astype(BF16).astype(F32)
        return total.astype(BF16)

    def finish(n):
        gone[n].wait_recv()
        PS[n] = (PS[n].astype(F32) + Q[n].astype(F32)).astype(BF16)
        outs[n].start()

    for n in range(N8):
        PX[n] = combine(1, n)
        gone[n].start()
    for n in range(N8):
        PS[n] = combine(0, n)
        finish(n)

    for cp in metas + own_y + own_x + [own_s] + fwd + y_s + x_s + d_s + sends + gone:
        cp.wait_send()
    for cp in outs:
        cp.wait()


def solution(mesh):
    row_spec = P(('dp', 'grp', 'ing'))
    exp_spec = P(('grp', 'ing'))

    def local_fn(tokens, expert_ids, gate_vals, w_one, w_three, w_two):
        ids = expert_ids.reshape(TOK, 4).T
        gates = gate_vals.reshape(TOK, 4).T
        dma = pltpu.SemaphoreType.DMA
        anywhere = pl.BlockSpec(memory_space=pl.ANY)
        vmem = pl.BlockSpec(memory_space=pltpu.VMEM)
        return pl.pallas_call(
            kernel,
            out_shape=jax.ShapeDtypeStruct((TOK, D), BF16),
            in_specs=[vmem, vmem, anywhere, anywhere, anywhere, anywhere],
            out_specs=anywhere,
            scratch_shapes=[
                pltpu.VMEM((NS, D, 2 * FC), BF16),
                pltpu.VMEM((4, 2 * TOK, D), BF16),
                pltpu.VMEM((EL, 8 * CAP, D), BF16),
                pltpu.VMEM((3, 8 * CAP, FF), BF16),
                pltpu.VMEM((N8, EL, 8 * CAP, NB), BF16),
                pltpu.VMEM((N8, 2, 2, EL, 2 * CAP, NB), BF16),
                pltpu.VMEM((N8, TOK, NB), BF16),
                pltpu.VMEM((N8, TOK, NB), BF16),
                pltpu.VMEM((N8, TOK, NB), BF16),
                pltpu.VMEM((2, 4 * TOK, TOK), BF16),
                pltpu.VMEM((8, TOK, TOK), F32),
                pltpu.VMEM((4, 128, 256), BF16),
                pltpu.VMEM((8, 8, TOK), F32),
                dma((NS,)), dma((NS,)), dma(()),
                dma((6, CH)), dma((6, CH)), dma((1,)), dma((1,)),
                dma((7,)), dma((7,)),
                dma((64,)), dma((64,)), dma((N8,)), dma((N8,)), dma((N8,)),
            ],
            compiler_params=pltpu.CompilerParams(collective_id=0, has_side_effects=True, vmem_limit_bytes=67043328),
        )(ids, gates, tokens, w_one, w_three, w_two)

    return jax.shard_map(local_fn, mesh=mesh, in_specs=(row_spec, row_spec, row_spec, exp_spec, exp_spec, exp_spec), out_specs=row_spec, check_vma=False)
```

```python
import functools

import jax
import jax.numpy as jnp
from jax import lax
from jax.experimental import pallas as pl
from jax.experimental.pallas import tpu as pltpu
from jax.sharding import PartitionSpec as P

MESH = pl.DeviceIdType.MESH
BF16 = jnp.bfloat16
F32 = jnp.float32
I32 = jnp.int32

TOK = 128
D = 2048
FF = 1792
EL = 4
CAP = 16
FC = 256
NF = FF // FC
NC = 512
N4 = D // NC
NB = 256
N8 = D // NB
CH = 4
CR = TOK // CH

NS = 24

BLOCK = {(1, 0, 0): 0, (1, 0, 1): 1, (0, 0, 0): 2, (0, 0, 1): 3,
         (0, 1, 0): 4, (0, 1, 1): 5, (1, 1, 0): 6, (1, 1, 1): 7}
NEAR = 6 * CAP
NEAR_PEERS = [(1, 0, 0), (0, 1, 0), (1, 0, 1), (0, 1, 1), (0, 0, 1)]
FAR_PEERS = [(1, 1, 0), (1, 1, 1)]

ORDER = (1, 0, 2, 3)
FETCH = []
for _e in ORDER:
    FETCH += [(1, _e, _f) for _f in range(NF)] + [(2, _e, _n) for _n in range(N4)]


def kernel(ids_ref, gate_ref, tok_hbm, w1, w3, w2, y_hbm,
           ring, T, X, act, E, R, PS, CM, GB, GH, META,
           ws_a, ws_b, tsem, bs, br, ss, sr, ms, mr, es, er, ysem):
    g = lax.axis_index('grp')
    y = lax.axis_index('ing')
    x = g // 2
    c = g % 2

    def peer(dy, dx, dc):
        return {'ing': (y + dy) % 2, 'grp': ((x + dx) % 2) * 2 + (c + dc) % 2}

    def remote(src, dst, s, r, to):
        return pltpu.make_async_remote_copy(src_ref=src, dst_ref=dst, send_sem=s, recv_sem=r, device_id=peer(*to), device_id_type=MESH)

    def w13(e, f, slot):
        col = pl.ds(pl.multiple_of(f * FC, FC), FC)
        return (pltpu.make_async_copy(w1.at[e, :, col], ring.at[slot, :, pl.ds(0, FC)], ws_a.at[slot]),
                pltpu.make_async_copy(w3.at[e, :, col], ring.at[slot, :, pl.ds(FC, FC)], ws_b.at[slot]))

    def w2c(e, n, slot):
        return (pltpu.make_async_copy(w2.at[e, :, pl.ds(n * NC, NC)], ring.at[slot, pl.ds(0, FF), :], ws_a.at[slot]),)

    def start(copies):
        for cp in copies:
            cp.start(priority=1)

    def wait(copies):
        for cp in copies:
            cp.wait()

    own = pltpu.make_async_copy(tok_hbm, T.at[0, pl.ds(0, TOK), :], tsem)
    own.start()
    slot_of = {}
    queue = list(FETCH)

    def fetch(chunk):
        layer, e, j = chunk
        return (w13 if layer == 1 else w2c)(e, j, slot_of[chunk])

    def refill(slot):
        if queue:
            chunk = queue.pop(0)
            slot_of[chunk] = slot
            start(fetch(chunk))

    for i in range(NS):
        refill(i)

    META[0] = jnp.concatenate([ids_ref[...].astype(F32), gate_ref[...]], axis=0)

    barrier = pltpu.get_barrier_semaphore()
    direct = [(0, 0, 1), (0, 1, 0), (1, 0, 0), (1, 0, 1)]
    for p in direct:
        pl.semaphore_signal(barrier, inc=1, device_id=peer(*p), device_id_type=MESH)
    pl.semaphore_wait(barrier, len(direct))

    metas = [remote(META.at[i], META.at[j], ms.at[k], mr.at[k], to) for k, (i, j, to) in enumerate([
        (0, 4, (1, 0, 0)), (0, 2, (0, 1, 0)), (0, 1, (0, 0, 1)),
        (4, 5, (0, 0, 1)), (4, 6, (0, 1, 0)), (2, 3, (0, 0, 1)), (6, 7, (0, 0, 1))])]
    for m in metas[:3]:
        m.start()
    own.wait()

    def rows(k):
        return pl.ds(k * CR, CR)

    def rows2(k):
        return pl.ds(TOK + k * CR, CR)

    own_y = [remote(T.at[0, rows(k)], T.at[2, rows(k)], bs.at[0, k], br.at[0, k], (1, 0, 0)) for k in range(CH)]
    own_x = [remote(T.at[0, rows(k)], T.at[1, rows(k)], bs.at[1, k], br.at[1, k], (0, 1, 0)) for k in range(CH)]
    own_s = remote(T.at[0, pl.ds(0, TOK)], T.at[0, pl.ds(TOK, TOK)], ss.at[0], sr.at[0], (0, 0, 1))
    fwd = [remote(T.at[2 if k < CH // 2 else 1, rows(k)], T.at[3, rows(k)], bs.at[2, k], br.at[2, k],
                  (0, 1, 0) if k < CH // 2 else (1, 0, 0)) for k in range(CH)]
    y_s = [remote(T.at[2, rows(k)], T.at[2, rows2(k)], bs.at[3, k], br.at[3, k], (0, 0, 1)) for k in range(CH)]
    x_s = [remote(T.at[1, rows(k)], T.at[1, rows2(k)], bs.at[4, k], br.at[4, k], (0, 0, 1)) for k in range(CH)]
    d_s = [remote(T.at[3, rows(k)], T.at[3, rows2(k)], bs.at[5, k], br.at[5, k], (0, 0, 1)) for k in range(CH)]
    own_y[0].start()
    own_x[0].start()
    metas[0].wait_recv()
    metas[4].start()
    metas[3].start()
    metas[1].wait_recv()
    metas[5].start()
    for k in range(1, CH):
        own_y[k].start()
        own_x[k].start()
    own_s.start()

    metas[4].wait_recv()
    metas[6].start()
    for i in (2, 3, 5, 6):
        metas[i].wait_recv()
    sub = lax.broadcasted_iota(I32, (TOK, TOK), 0)
    lane = lax.broadcasted_iota(I32, (TOK, TOK), 1)
    base = ((g * 2 + y) * EL).astype(F32)
    hot_rows = []
    for h in range(8):
        ids_h = META[h][0:4, :]
        for e in range(EL):
            hot_rows.append(jnp.sum(jnp.where(ids_h == base + e, 1.0, 0.0), axis=0, keepdims=True))
    hot = jnp.concatenate(hot_rows, axis=0)
    rank = jnp.dot(hot.astype(BF16), (sub < lane).astype(BF16), preferred_element_type=F32)
    key = jnp.where(hot > 0.0, rank, -1.0)
    slot16 = lax.broadcasted_iota(I32, (CAP, TOK), 0).astype(F32)
    zero16 = jnp.zeros((CAP, TOK), F32)
    for q in range(4):
        parts = []
        for e in range(EL):
            for dc in range(2):
                r = (q * 2 + dc) * EL + e
                hit = jnp.where(key[r:r + 1, :] == slot16, 1.0, 0.0)
                parts.append(jnp.concatenate([hit, zero16] if dc == 0 else [zero16, hit], axis=1))
        GH[q] = jnp.concatenate(parts, axis=0).astype(BF16)

    lower = (lane < sub).astype(BF16)
    lane_f = lane.astype(F32)
    meta_t = jnp.transpose(jnp.concatenate([META[0], jnp.zeros((TOK - 8, TOK), F32)], axis=0))
    ids_c = [meta_t[:, k:k + 1] for k in range(4)]
    gate_c = [meta_t[:, 4 + k:5 + k] for k in range(4)]
    hot_t = sum(jnp.where(ids_c[k] == lane_f, 1.0, 0.0) for k in range(4))
    rank_t = jnp.dot(lower, hot_t.astype(BF16), preferred_element_type=F32)
    row_of, grp_of = [], []
    for k in range(4):
        slot = jnp.sum(jnp.where(ids_c[k] == lane_f, rank_t, 0.0), axis=1, keepdims=True).astype(I32)
        idi = ids_c[k].astype(I32)
        row_of.append((((idi >> 2) + y) & 1) * 64 + (idi & 3) * CAP + slot)
        grp_of.append((((idi >> 4) + x) & 1) * 2 + (((idi >> 3) + c) & 1))
    for r in range(4):
        for u in range(2):
            sel = [grp_of[2 * m + u] == r for m in range(2)]
            row = jnp.where(sel[0], row_of[u], jnp.where(sel[1], row_of[2 + u], -1))
            gate = jnp.where(sel[0], gate_c[u], jnp.where(sel[1], gate_c[2 + u], 0.0))
            CM[r, u * TOK:(u + 1) * TOK, :] = jnp.where(row == lane, 1.0, 0.0).astype(BF16)
            GB[r * 2 + u] = jnp.broadcast_to(gate, (TOK, TOK))

    def gather(q):
        dy, dx = q // 2, q % 2
        for n in range(N4):
            cols = pl.ds(n * NC, NC)
            got = jnp.dot(GH[q], T[q, :, cols], preferred_element_type=F32).astype(BF16)
            for e in range(EL):
                for dc in range(2):
                    i = (e * 2 + dc) * CAP
                    X[e, pl.ds(BLOCK[(dy, dx, dc)] * CAP, CAP), cols] = got[i:i + CAP, :]

    def far(k):
        fwd[k].wait_recv()
        d_s[k].start()

    for k in range(CH):
        own_y[k].wait_recv()
        y_s[k].start()
        if k < CH // 2:
            fwd[k].start()
        own_x[k].wait_recv()
        x_s[k].start()
        if k >= CH // 2:
            fwd[k].start()
    own_s.wait_recv()
    gather(0)
    for k in range(CH):
        y_s[k].wait_recv()
        x_s[k].wait_recv()
    gather(1)
    gather(2)

    waited = set()

    def layer1(chunk, r0, r1):
        _, e, f = chunk
        h = jnp.dot(X[e, r0:r1, :], ring[slot_of[chunk]], preferred_element_type=F32)
        h1 = h[:, :FC]
        act[e % 2, r0:r1, f * FC:(f + 1) * FC] = (jax.nn.silu(h1) * h[:, FC:]).astype(BF16)

    def layer2(chunk, r0, r1):
        _, e, n = chunk
        out = jnp.dot(act[e % 2, r0:r1, :], ring[slot_of[chunk], 0:FF, :], preferred_element_type=F32).astype(BF16)
        for t in range(2):
            blk = out[:, t * NB:(t + 1) * NB]
            E[2 * n + t, e, r0:r1, :] = blk
            if r0 == 0:
                R[2 * n + t, 0, 0, e] = blk[32:48, :]

    def run(todo, last=True):
        for chunk, _, _ in todo:
            if chunk not in waited:
                waited.add(chunk)
                wait(fetch(chunk))
        for chunk, r0, r1 in todo:
            (layer1 if chunk[0] == 1 else layer2)(chunk, r0, r1)
        if last:
            for chunk, _, _ in todo:
                refill(slot_of[chunk])

    sends = []
    arrive = [[] for n in range(N8)]

    def send(peers, n0, nn, e):
        for p in peers:
            dy, dx, dc = p
            k = len(sends)
            cp = remote(E.at[pl.ds(n0, nn), e, pl.ds(BLOCK[p] * CAP, CAP), :],
                        R.at[pl.ds(n0, nn), dx * 2 + dc, dy, e], es.at[k], er.at[k], p)
            cp.start()
            sends.append(cp)
            arrive[n0].append(cp)

    def l1(e, lo, hi, r0=0, r1=8 * CAP):
        return [((1, e, f), r0, r1) for f in range(lo, hi)]

    def l2(e, lo, hi, r0=0, r1=8 * CAP):
        return [((2, e, n), r0, r1) for n in range(lo, hi)]

    def far(k):
        fwd[k].wait_recv()
        d_s[k].start()

    first = ORDER[0]
    run(l1(first, 0, NF, 0, NEAR), False)
    far(0)
    far(2)
    run(l2(first, 0, N4, 0, NEAR), False)
    send(NEAR_PEERS, 0, N8, first)
    far(1)
    far(3)
    for k in range(CH):
        d_s[k].wait_recv()
    gather(3)
    run(l1(first, 0, 3, NEAR))
    run(l1(first, 3, NF, NEAR))
    run(l2(first, 0, N4, NEAR))
    send(FAR_PEERS, 0, N8, first)
    for e in ORDER[1:3]:
        run(l1(e, 0, NF))
        for n in (0, 2):
            run(l2(e, n, n + 2))
            send(FAR_PEERS + NEAR_PEERS, 2 * n, 4, e)
    last = ORDER[3]
    run(l1(last, 0, 4))
    run(l1(last, 4, NF))
    for n in range(N4):
        run(l2(last, n, n + 1))
        send(FAR_PEERS + NEAR_PEERS, 2 * n, 2, last)

    outs = [pltpu.make_async_copy(PS.at[n], y_hbm.at[:, pl.ds(n * NB, NB)], ysem.at[n]) for n in range(N8)]
    for n in range(N8):
        for cp in arrive[n]:
            cp.wait_recv()
        total = jnp.zeros((TOK, NB), F32)
        for r in range(4):
            part = jnp.dot(CM[r], R[n, r].reshape(128, NB), preferred_element_type=F32)
            g0 = GB[r * 2]
            g1 = GB[r * 2 + 1]
            g0 = jnp.concatenate([g0, g0], axis=1)
            g1 = jnp.concatenate([g1, g1], axis=1)
            total = total + (g0 * part[:TOK] + g1 * part[TOK:]).astype(BF16).astype(F32)
        PS[n] = total.astype(BF16)
        outs[n].start()

    for cp in metas + own_y + own_x + [own_s] + fwd + y_s + x_s + d_s + sends:
        cp.wait_send()
    for cp in outs:
        cp.wait()


def solution(mesh):
    row_spec = P(('dp', 'grp', 'ing'))
    exp_spec = P(('grp', 'ing'))

    def local_fn(tokens, expert_ids, gate_vals, w_one, w_three, w_two):
        ids = expert_ids.reshape(TOK, 4).T
        gates = gate_vals.reshape(TOK, 4).T
        dma = pltpu.SemaphoreType.DMA
        anywhere = pl.BlockSpec(memory_space=pl.ANY)
        vmem = pl.BlockSpec(memory_space=pltpu.VMEM)
        return pl.pallas_call(
            kernel,
            out_shape=jax.ShapeDtypeStruct((TOK, D), BF16),
            in_specs=[vmem, vmem, anywhere, anywhere, anywhere, anywhere],
            out_specs=anywhere,
            scratch_shapes=[
                pltpu.VMEM((NS, D, 2 * FC), BF16),
                pltpu.VMEM((4, 2 * TOK, D), BF16),
                pltpu.VMEM((EL, 8 * CAP, D), BF16),
                pltpu.VMEM((2, 8 * CAP, FF), BF16),
                pltpu.VMEM((N8, EL, 8 * CAP, NB), BF16),
                pltpu.VMEM((N8, 4, 2, EL, CAP, NB), BF16),
                pltpu.VMEM((N8, TOK, NB), BF16),
                pltpu.VMEM((4, 2 * TOK, TOK), BF16),
                pltpu.VMEM((8, TOK, TOK), F32),
                pltpu.VMEM((4, 128, 256), BF16),
                pltpu.VMEM((8, 8, TOK), F32),
                dma((NS,)), dma((NS,)), dma(()),
                dma((6, CH)), dma((6, CH)), dma((1,)), dma((1,)),
                dma((7,)), dma((7,)),
                dma((72,)), dma((72,)), dma((N8,)),
            ],
            compiler_params=pltpu.CompilerParams(collective_id=0, has_side_effects=True, vmem_limit_bytes=67043328),
        )(ids, gates, tokens, w_one, w_three, w_two)

    return jax.shard_map(local_fn, mesh=mesh, in_specs=(row_spec, row_spec, row_spec, exp_spec, exp_spec, exp_spec), out_specs=row_spec, check_vma=False)
```

```python
import functools

import jax
import jax.numpy as jnp
from jax import lax
from jax.experimental import pallas as pl
from jax.experimental.pallas import tpu as pltpu
from jax.sharding import PartitionSpec as P

MESH = pl.DeviceIdType.MESH
BF16 = jnp.bfloat16
F32 = jnp.float32
I32 = jnp.int32

TOK = 128
D = 2048
FF = 1792
EL = 4
CAP = 16
FC = 256
NF = FF // FC
NC = 512
N4 = D // NC
NB = 256
N8 = D // NB
CH = 4
CR = TOK // CH

NS = 23

BLOCK = {(1, 0, 0): 0, (1, 0, 1): 1, (0, 0, 0): 2, (0, 0, 1): 3,
         (0, 1, 0): 4, (0, 1, 1): 5, (1, 1, 0): 6, (1, 1, 1): 7}
NEAR = 6 * CAP
NEAR_PEERS = [(1, 0, 0), (0, 1, 0), (1, 0, 1), (0, 1, 1), (0, 0, 1)]
FAR_PEERS = [(1, 1, 0), (1, 1, 1)]

ORDER = (1, 0, 2, 3)
FETCH = []
for _e in ORDER:
    FETCH += [(1, _e, _f) for _f in range(NF)] + [(2, _e, _n) for _n in range(N4)]


def kernel(ids_ref, gate_ref, tok_hbm, w1, w3, w2, y_ref,
           ring, T, X, act, E, R, CM, GB, GH, META,
           ws_a, ws_b, tsem, bs, br, ss, sr, ms, mr, es, er):
    g = lax.axis_index('grp')
    y = lax.axis_index('ing')
    x = g // 2
    c = g % 2

    def peer(dy, dx, dc):
        return {'ing': (y + dy) % 2, 'grp': ((x + dx) % 2) * 2 + (c + dc) % 2}

    def remote(src, dst, s, r, to):
        return pltpu.make_async_remote_copy(src_ref=src, dst_ref=dst, send_sem=s, recv_sem=r, device_id=peer(*to), device_id_type=MESH)

    def w13(e, f, slot):
        col = pl.ds(pl.multiple_of(f * FC, FC), FC)
        return (pltpu.make_async_copy(w1.at[e, :, col], ring.at[slot, :, pl.ds(0, FC)], ws_a.at[slot]),
                pltpu.make_async_copy(w3.at[e, :, col], ring.at[slot, :, pl.ds(FC, FC)], ws_b.at[slot]))

    def w2c(e, n, slot):
        return (pltpu.make_async_copy(w2.at[e, :, pl.ds(n * NC, NC)], ring.at[slot, pl.ds(0, FF), :], ws_a.at[slot]),)

    def start(copies):
        for cp in copies:
            cp.start(priority=1)

    def wait(copies):
        for cp in copies:
            cp.wait()

    own = pltpu.make_async_copy(tok_hbm, T.at[0, pl.ds(0, TOK), :], tsem)
    own.start()
    slot_of = {}
    queue = list(FETCH)

    def fetch(chunk):
        layer, e, j = chunk
        return (w13 if layer == 1 else w2c)(e, j, slot_of[chunk])

    def refill(slot):
        if queue:
            chunk = queue.pop(0)
            slot_of[chunk] = slot
            start(fetch(chunk))

    for i in range(NS):
        refill(i)

    META[0] = jnp.concatenate([ids_ref[...].astype(F32), gate_ref[...]], axis=0)

    barrier = pltpu.get_barrier_semaphore()
    direct = [(0, 0, 1), (0, 1, 0), (1, 0, 0), (1, 0, 1)]
    for p in direct:
        pl.semaphore_signal(barrier, inc=1, device_id=peer(*p), device_id_type=MESH)
    pl.semaphore_wait(barrier, len(direct))

    metas = [remote(META.at[i], META.at[j], ms.at[k], mr.at[k], to) for k, (i, j, to) in enumerate([
        (0, 4, (1, 0, 0)), (0, 2, (0, 1, 0)), (0, 1, (0, 0, 1)),
        (4, 5, (0, 0, 1)), (4, 6, (0, 1, 0)), (2, 3, (0, 0, 1)), (6, 7, (0, 0, 1))])]
    for m in metas[:3]:
        m.start()
    own.wait()

    def rows(k):
        return pl.ds(k * CR, CR)

    def rows2(k):
        return pl.ds(TOK + k * CR, CR)

    own_y = [remote(T.at[0, rows(k)], T.at[2, rows(k)], bs.at[0, k], br.at[0, k], (1, 0, 0)) for k in range(CH)]
    own_x = [remote(T.at[0, rows(k)], T.at[1, rows(k)], bs.at[1, k], br.at[1, k], (0, 1, 0)) for k in range(CH)]
    own_s = remote(T.at[0, pl.ds(0, TOK)], T.at[0, pl.ds(TOK, TOK)], ss.at[0], sr.at[0], (0, 0, 1))
    fwd = [remote(T.at[2 if k < CH // 2 else 1, rows(k)], T.at[3, rows(k)], bs.at[2, k], br.at[2, k],
                  (0, 1, 0) if k < CH // 2 else (1, 0, 0)) for k in range(CH)]
    y_s = [remote(T.at[2, rows(k)], T.at[2, rows2(k)], bs.at[3, k], br.at[3, k], (0, 0, 1)) for k in range(CH)]
    x_s = [remote(T.at[1, rows(k)], T.at[1, rows2(k)], bs.at[4, k], br.at[4, k], (0, 0, 1)) for k in range(CH)]
    d_s = [remote(T.at[3, rows(k)], T.at[3, rows2(k)], bs.at[5, k], br.at[5, k], (0, 0, 1)) for k in range(CH)]
    own_y[0].start()
    own_x[0].start()
    metas[0].wait_recv()
    metas[4].start()
    metas[3].start()
    metas[1].wait_recv()
    metas[5].start()
    for k in range(1, CH):
        own_y[k].start()
        own_x[k].start()
    own_s.start()

    metas[4].wait_recv()
    metas[6].start()
    for i in (2, 3, 5, 6):
        metas[i].wait_recv()
    sub = lax.broadcasted_iota(I32, (TOK, TOK), 0)
    lane = lax.broadcasted_iota(I32, (TOK, TOK), 1)
    base = ((g * 2 + y) * EL).astype(F32)
    hot_rows = []
    for h in range(8):
        ids_h = META[h][0:4, :]
        for e in range(EL):
            hot_rows.append(jnp.sum(jnp.where(ids_h == base + e, 1.0, 0.0), axis=0, keepdims=True))
    hot = jnp.concatenate(hot_rows, axis=0)
    rank = jnp.dot(hot.astype(BF16), (sub < lane).astype(BF16), preferred_element_type=F32)
    key = jnp.where(hot > 0.0, rank, -1.0)
    slot16 = lax.broadcasted_iota(I32, (CAP, TOK), 0).astype(F32)
    zero16 = jnp.zeros((CAP, TOK), F32)
    for q in range(4):
        parts = []
        for e in range(EL):
            for dc in range(2):
                r = (q * 2 + dc) * EL + e
                hit = jnp.where(key[r:r + 1, :] == slot16, 1.0, 0.0)
                parts.append(jnp.concatenate([hit, zero16] if dc == 0 else [zero16, hit], axis=1))
        GH[q] = jnp.concatenate(parts, axis=0).astype(BF16)

    lower = (lane < sub).astype(BF16)
    lane_f = lane.astype(F32)
    meta_t = jnp.transpose(jnp.concatenate([META[0], jnp.zeros((TOK - 8, TOK), F32)], axis=0))
    ids_c = [meta_t[:, k:k + 1] for k in range(4)]
    gate_c = [meta_t[:, 4 + k:5 + k] for k in range(4)]
    hot_t = sum(jnp.where(ids_c[k] == lane_f, 1.0, 0.0) for k in range(4))
    rank_t = jnp.dot(lower, hot_t.astype(BF16), preferred_element_type=F32)
    row_of, grp_of = [], []
    for k in range(4):
        slot = jnp.sum(jnp.where(ids_c[k] == lane_f, rank_t, 0.0), axis=1, keepdims=True).astype(I32)
        idi = ids_c[k].astype(I32)
        row_of.append((((idi >> 2) + y) & 1) * 64 + (idi & 3) * CAP + slot)
        grp_of.append((((idi >> 4) + x) & 1) * 2 + (((idi >> 3) + c) & 1))
    for r in range(4):
        for u in range(2):
            sel = [grp_of[2 * m + u] == r for m in range(2)]
            row = jnp.where(sel[0], row_of[u], jnp.where(sel[1], row_of[2 + u], -1))
            gate = jnp.where(sel[0], gate_c[u], jnp.where(sel[1], gate_c[2 + u], 0.0))
            CM[r, u * TOK:(u + 1) * TOK, :] = jnp.where(row == lane, 1.0, 0.0).astype(BF16)
            GB[r * 2 + u] = jnp.broadcast_to(gate, (TOK, TOK))

    def gather(q):
        dy, dx = q // 2, q % 2
        for n in range(N4):
            cols = pl.ds(n * NC, NC)
            got = jnp.dot(GH[q], T[q, :, cols], preferred_element_type=F32).astype(BF16)
            for e in range(EL):
                for dc in range(2):
                    i = (e * 2 + dc) * CAP
                    X[e, pl.ds(BLOCK[(dy, dx, dc)] * CAP, CAP), cols] = got[i:i + CAP, :]

    def far(k):
        fwd[k].wait_recv()
        d_s[k].start()

    for k in range(CH):
        own_y[k].wait_recv()
        y_s[k].start()
        if k < CH // 2:
            fwd[k].start()
        own_x[k].wait_recv()
        x_s[k].start()
        if k >= CH // 2:
            fwd[k].start()
    own_s.wait_recv()
    gather(0)
    for k in range(CH):
        y_s[k].wait_recv()
        x_s[k].wait_recv()
    gather(1)
    gather(2)

    waited = set()

    def layer1(chunk, r0, r1):
        _, e, f = chunk
        h = jnp.dot(X[e, r0:r1, :], ring[slot_of[chunk]], preferred_element_type=F32)
        h1 = h[:, :FC]
        act[e % 2, r0:r1, f * FC:(f + 1) * FC] = (jax.nn.silu(h1) * h[:, FC:]).astype(BF16)

    def layer2(chunk, r0, r1):
        _, e, n = chunk
        out = jnp.dot(act[e % 2, r0:r1, :], ring[slot_of[chunk], 0:FF, :], preferred_element_type=F32).astype(BF16)
        for t in range(2):
            blk = out[:, t * NB:(t + 1) * NB]
            E[2 * n + t, e, r0:r1, :] = blk
            if r0 == 0:
                R[2 * n + t, 0, 0, e] = blk[32:48, :]

    def run(todo, last=True):
        for chunk, _, _ in todo:
            if chunk not in waited:
                waited.add(chunk)
                wait(fetch(chunk))
        for chunk, r0, r1 in todo:
            (layer1 if chunk[0] == 1 else layer2)(chunk, r0, r1)
        if last:
            for chunk, _, _ in todo:
                refill(slot_of[chunk])

    sends = []
    arrive = [[] for n in range(N8)]

    def send(peers, n0, nn, e):
        for p in peers:
            dy, dx, dc = p
            k = len(sends)
            cp = remote(E.at[pl.ds(n0, nn), e, pl.ds(BLOCK[p] * CAP, CAP), :],
                        R.at[pl.ds(n0, nn), dx * 2 + dc, dy, e], es.at[k], er.at[k], p)
            cp.start()
            sends.append(cp)
            arrive[n0].append(cp)

    def l1(e, lo, hi, r0=0, r1=8 * CAP):
        return [((1, e, f), r0, r1) for f in range(lo, hi)]

    def l2(e, lo, hi, r0=0, r1=8 * CAP):
        return [((2, e, n), r0, r1) for n in range(lo, hi)]

    def far(k):
        fwd[k].wait_recv()
        d_s[k].start()

    first = ORDER[0]
    run(l1(first, 0, NF, 0, NEAR), False)
    far(0)
    far(2)
    run(l2(first, 0, N4, 0, NEAR), False)
    send(NEAR_PEERS, 0, N8, first)
    far(1)
    far(3)
    for k in range(CH):
        d_s[k].wait_recv()
    gather(3)
    def whole(e, cuts):
        run(l1(e, 0, NF))
        for lo, hi in cuts:
            run(l2(e, lo, hi))
            send(FAR_PEERS + NEAR_PEERS, 2 * lo, 2 * (hi - lo), e)

    whole(ORDER[1], ((0, 1), (1, 2), (2, 4)))
    run(l1(first, 0, NF, NEAR))
    run(l2(first, 0, N4, NEAR))
    send(FAR_PEERS, 0, N8, first)
    whole(ORDER[2], ((0, 2), (2, 4)))
    last = ORDER[3]
    run(l1(last, 0, 4))
    run(l1(last, 4, NF))
    for n in range(N4):
        run(l2(last, n, n + 1))
        send(FAR_PEERS + NEAR_PEERS, 2 * n, 2, last)

    for n in range(N8):
        for cp in arrive[n]:
            cp.wait_recv()
        total = jnp.zeros((TOK, NB), F32)
        for r in range(4):
            part = jnp.dot(CM[r], R[n, r].reshape(128, NB), preferred_element_type=F32)
            g0 = GB[r * 2]
            g1 = GB[r * 2 + 1]
            g0 = jnp.concatenate([g0, g0], axis=1)
            g1 = jnp.concatenate([g1, g1], axis=1)
            total = total + (g0 * part[:TOK] + g1 * part[TOK:]).astype(BF16).astype(F32)
        y_ref[:, n * NB:(n + 1) * NB] = total.astype(BF16)

    for cp in metas + own_y + own_x + [own_s] + fwd + y_s + x_s + d_s + sends:
        cp.wait_send()


def solution(mesh):
    row_spec = P(('dp', 'grp', 'ing'))
    exp_spec = P(('grp', 'ing'))

    def local_fn(tokens, expert_ids, gate_vals, w_one, w_three, w_two):
        ids = expert_ids.reshape(TOK, 4).T
        gates = gate_vals.reshape(TOK, 4).T
        dma = pltpu.SemaphoreType.DMA
        anywhere = pl.BlockSpec(memory_space=pl.ANY)
        vmem = pl.BlockSpec(memory_space=pltpu.VMEM)
        return pl.pallas_call(
            kernel,
            out_shape=pltpu.VMEM((TOK, D), BF16),
            in_specs=[vmem, vmem, anywhere, anywhere, anywhere, anywhere],
            out_specs=vmem,
            scratch_shapes=[
                pltpu.VMEM((NS, D, 2 * FC), BF16),
                pltpu.VMEM((4, 2 * TOK, D), BF16),
                pltpu.VMEM((EL, 8 * CAP, D), BF16),
                pltpu.VMEM((2, 8 * CAP, FF), BF16),
                pltpu.VMEM((N8, EL, 8 * CAP, NB), BF16),
                pltpu.VMEM((N8, 4, 2, EL, CAP, NB), BF16),
                pltpu.VMEM((4, 2 * TOK, TOK), BF16),
                pltpu.VMEM((8, TOK, TOK), F32),
                pltpu.VMEM((4, 128, 256), BF16),
                pltpu.VMEM((8, 8, TOK), F32),
                dma((NS,)), dma((NS,)), dma(()),
                dma((6, CH)), dma((6, CH)), dma((1,)), dma((1,)),
                dma((7,)), dma((7,)),
                dma((72,)), dma((72,)),
            ],
            compiler_params=pltpu.CompilerParams(collective_id=0, has_side_effects=True, vmem_limit_bytes=65000000),
        )(ids, gates, tokens, w_one, w_three, w_two)

    return jax.shard_map(local_fn, mesh=mesh, in_specs=(row_spec, row_spec, row_spec, exp_spec, exp_spec, exp_spec), out_specs=row_spec, check_vma=False)
```

```python
import functools

import jax
import jax.numpy as jnp
from jax import lax
from jax.experimental import pallas as pl
from jax.experimental.pallas import tpu as pltpu
from jax.sharding import PartitionSpec as P

MESH = pl.DeviceIdType.MESH
BF16 = jnp.bfloat16
F32 = jnp.float32
I32 = jnp.int32

TOK = 128
D = 2048
FF = 1792
EL = 4
CAP = 16
FC = 256
NF = FF // FC
NC = 512
N4 = D // NC
NB = 256
N8 = D // NB
CH = 4
CR = TOK // CH

NS = 23

BLOCK = {(1, 0, 0): 0, (1, 0, 1): 1, (0, 0, 0): 2, (0, 0, 1): 3,
         (0, 1, 0): 4, (0, 1, 1): 5, (1, 1, 0): 6, (1, 1, 1): 7}
NEAR = 6 * CAP
NEAR_PEERS = [(1, 0, 0), (0, 1, 0), (1, 0, 1), (0, 1, 1), (0, 0, 1)]
FAR_PEERS = [(1, 1, 0), (1, 1, 1)]

ORDER = (1, 0, 2, 3)
FETCH = []
for _e in ORDER:
    FETCH += [(1, _e, _f) for _f in range(NF)] + [(2, _e, _n) for _n in range(N4)]


def kernel(ids_hbm, gate_hbm, tok_hbm, w1, w3, w2, y_ref,
           ids_ref, gate_ref, ring, T, X, act, E, R, CM, GB, GH, META,
           ws_a, ws_b, tsem, isem, bs, br, ss, sr, ms, mr, es, er):
    g = lax.axis_index('grp')
    y = lax.axis_index('ing')
    x = g // 2
    c = g % 2

    def peer(dy, dx, dc):
        return {'ing': (y + dy) % 2, 'grp': ((x + dx) % 2) * 2 + (c + dc) % 2}

    def remote(src, dst, s, r, to):
        return pltpu.make_async_remote_copy(src_ref=src, dst_ref=dst, send_sem=s, recv_sem=r, device_id=peer(*to), device_id_type=MESH)

    def w13(e, f, slot):
        col = pl.ds(pl.multiple_of(f * FC, FC), FC)
        return (pltpu.make_async_copy(w1.at[e, :, col], ring.at[slot, :, pl.ds(0, FC)], ws_a.at[slot]),
                pltpu.make_async_copy(w3.at[e, :, col], ring.at[slot, :, pl.ds(FC, FC)], ws_b.at[slot]))

    def w2c(e, n, slot):
        return (pltpu.make_async_copy(w2.at[e, :, pl.ds(n * NC, NC)], ring.at[slot, pl.ds(0, FF), :], ws_a.at[slot]),)

    def start(copies):
        for cp in copies:
            cp.start(priority=1)

    def wait(copies):
        for cp in copies:
            cp.wait()

    own = pltpu.make_async_copy(tok_hbm, T.at[0, pl.ds(0, TOK), :], tsem)
    small = [pltpu.make_async_copy(ids_hbm, ids_ref, isem.at[0]), pltpu.make_async_copy(gate_hbm, gate_ref, isem.at[1])]
    for cp in small:
        cp.start()
    own.start()
    slot_of = {}
    queue = list(FETCH)

    def fetch(chunk):
        layer, e, j = chunk
        return (w13 if layer == 1 else w2c)(e, j, slot_of[chunk])

    def refill(slot):
        if queue:
            chunk = queue.pop(0)
            slot_of[chunk] = slot
            start(fetch(chunk))

    for i in range(NS):
        refill(i)

    barrier = pltpu.get_barrier_semaphore()
    direct = [(0, 0, 1), (0, 1, 0), (1, 0, 0), (1, 0, 1)]
    for p in direct:
        pl.semaphore_signal(barrier, inc=1, device_id=peer(*p), device_id_type=MESH)
    for cp in small:
        cp.wait()
    META[0] = jnp.concatenate([ids_ref[...].astype(F32), gate_ref[...]], axis=0)
    pl.semaphore_wait(barrier, len(direct))

    metas = [remote(META.at[i], META.at[j], ms.at[k], mr.at[k], to) for k, (i, j, to) in enumerate([
        (0, 4, (1, 0, 0)), (0, 2, (0, 1, 0)), (0, 1, (0, 0, 1)),
        (4, 5, (0, 0, 1)), (4, 6, (0, 1, 0)), (2, 3, (0, 0, 1)), (6, 7, (0, 0, 1))])]
    for m in metas[:3]:
        m.start()
    own.wait()

    def rows(k):
        return pl.ds(k * CR, CR)

    def rows2(k):
        return pl.ds(TOK + k * CR, CR)

    own_y = [remote(T.at[0, rows(k)], T.at[2, rows(k)], bs.at[0, k], br.at[0, k], (1, 0, 0)) for k in range(CH)]
    own_x = [remote(T.at[0, rows(k)], T.at[1, rows(k)], bs.at[1, k], br.at[1, k], (0, 1, 0)) for k in range(CH)]
    own_s = remote(T.at[0, pl.ds(0, TOK)], T.at[0, pl.ds(TOK, TOK)], ss.at[0], sr.at[0], (0, 0, 1))
    fwd = [remote(T.at[2 if k < CH // 2 else 1, rows(k)], T.at[3, rows(k)], bs.at[2, k], br.at[2, k],
                  (0, 1, 0) if k < CH // 2 else (1, 0, 0)) for k in range(CH)]
    y_s = [remote(T.at[2, rows(k)], T.at[2, rows2(k)], bs.at[3, k], br.at[3, k], (0, 0, 1)) for k in range(CH)]
    x_s = [remote(T.at[1, rows(k)], T.at[1, rows2(k)], bs.at[4, k], br.at[4, k], (0, 0, 1)) for k in range(CH)]
    d_s = [remote(T.at[3, rows(k)], T.at[3, rows2(k)], bs.at[5, k], br.at[5, k], (0, 0, 1)) for k in range(CH)]
    own_y[0].start()
    own_x[0].start()
    metas[0].wait_recv()
    metas[4].start()
    metas[3].start()
    metas[1].wait_recv()
    metas[5].start()
    for k in range(1, CH):
        own_y[k].start()
        own_x[k].start()
    own_s.start()

    metas[4].wait_recv()
    metas[6].start()
    for i in (2, 3, 5, 6):
        metas[i].wait_recv()
    sub = lax.broadcasted_iota(I32, (TOK, TOK), 0)
    lane = lax.broadcasted_iota(I32, (TOK, TOK), 1)
    base = ((g * 2 + y) * EL).astype(F32)
    hot_rows = []
    for h in range(8):
        ids_h = META[h][0:4, :]
        for e in range(EL):
            hot_rows.append(jnp.sum(jnp.where(ids_h == base + e, 1.0, 0.0), axis=0, keepdims=True))
    hot = jnp.concatenate(hot_rows, axis=0)
    rank = jnp.dot(hot.astype(BF16), (sub < lane).astype(BF16), preferred_element_type=F32)
    key = jnp.where(hot > 0.0, rank, -1.0)
    slot16 = lax.broadcasted_iota(I32, (CAP, TOK), 0).astype(F32)
    zero16 = jnp.zeros((CAP, TOK), F32)
    for q in range(4):
        parts = []
        for e in range(EL):
            for dc in range(2):
                r = (q * 2 + dc) * EL + e
                hit = jnp.where(key[r:r + 1, :] == slot16, 1.0, 0.0)
                parts.append(jnp.concatenate([hit, zero16] if dc == 0 else [zero16, hit], axis=1))
        GH[q] = jnp.concatenate(parts, axis=0).astype(BF16)

    lower = (lane < sub).astype(BF16)
    lane_f = lane.astype(F32)
    meta_t = jnp.transpose(jnp.concatenate([META[0], jnp.zeros((TOK - 8, TOK), F32)], axis=0))
    ids_c = [meta_t[:, k:k + 1] for k in range(4)]
    gate_c = [meta_t[:, 4 + k:5 + k] for k in range(4)]
    hot_t = sum(jnp.where(ids_c[k] == lane_f, 1.0, 0.0) for k in range(4))
    rank_t = jnp.dot(lower, hot_t.astype(BF16), preferred_element_type=F32)
    row_of, grp_of = [], []
    for k in range(4):
        slot = jnp.sum(jnp.where(ids_c[k] == lane_f, rank_t, 0.0), axis=1, keepdims=True).astype(I32)
        idi = ids_c[k].astype(I32)
        row_of.append((((idi >> 2) + y) & 1) * 64 + (idi & 3) * CAP + slot)
        grp_of.append((((idi >> 4) + x) & 1) * 2 + (((idi >> 3) + c) & 1))
    for r in range(4):
        for u in range(2):
            sel = [grp_of[2 * m + u] == r for m in range(2)]
            row = jnp.where(sel[0], row_of[u], jnp.where(sel[1], row_of[2 + u], -1))
            gate = jnp.where(sel[0], gate_c[u], jnp.where(sel[1], gate_c[2 + u], 0.0))
            CM[r, u * TOK:(u + 1) * TOK, :] = jnp.where(row == lane, 1.0, 0.0).astype(BF16)
            GB[r * 2 + u] = jnp.broadcast_to(gate, (TOK, TOK))

    def gather(q):
        dy, dx = q // 2, q % 2
        for n in range(N4):
            cols = pl.ds(n * NC, NC)
            got = jnp.dot(GH[q], T[q, :, cols], preferred_element_type=F32).astype(BF16)
            for e in range(EL):
                for dc in range(2):
                    i = (e * 2 + dc) * CAP
                    X[e, pl.ds(BLOCK[(dy, dx, dc)] * CAP, CAP), cols] = got[i:i + CAP, :]

    def far(k):
        fwd[k].wait_recv()
        d_s[k].start()

    for k in range(CH):
        own_y[k].wait_recv()
        y_s[k].start()
        if k < CH // 2:
            fwd[k].start()
        own_x[k].wait_recv()
        x_s[k].start()
        if k >= CH // 2:
            fwd[k].start()
    own_s.wait_recv()
    gather(0)
    for k in range(CH):
        y_s[k].wait_recv()
        x_s[k].wait_recv()
    gather(1)
    gather(2)

    waited = set()

    def layer1(chunk, r0, r1):
        _, e, f = chunk
        h = jnp.dot(X[e, r0:r1, :], ring[slot_of[chunk]], preferred_element_type=F32)
        h1 = h[:, :FC]
        act[e % 2, r0:r1, f * FC:(f + 1) * FC] = (jax.nn.silu(h1) * h[:, FC:]).astype(BF16)

    def layer2(chunk, r0, r1):
        _, e, n = chunk
        out = jnp.dot(act[e % 2, r0:r1, :], ring[slot_of[chunk], 0:FF, :], preferred_element_type=F32).astype(BF16)
        for t in range(2):
            blk = out[:, t * NB:(t + 1) * NB]
            E[e, r0 // CAP:r1 // CAP, 2 * n + t] = blk.reshape((r1 - r0) // CAP, CAP, NB)
            if r0 == 0:
                R[0, 0, e, 2 * n + t] = blk[32:48, :]

    def run(todo, last=True):
        for chunk, _, _ in todo:
            if chunk not in waited:
                waited.add(chunk)
                wait(fetch(chunk))
        for chunk, r0, r1 in todo:
            (layer1 if chunk[0] == 1 else layer2)(chunk, r0, r1)
        if last:
            for chunk, _, _ in todo:
                refill(slot_of[chunk])

    sends = []
    arrive = [[] for n in range(N8)]

    def send(peers, n0, nn, e):
        for p in peers:
            dy, dx, dc = p
            k = len(sends)
            cp = remote(E.at[e, BLOCK[p], pl.ds(n0, nn)], R.at[dx * 2 + dc, dy, e, pl.ds(n0, nn)], es.at[k], er.at[k], p)
            cp.start()
            sends.append(cp)
            arrive[n0].append(cp)

    def l1(e, lo, hi, r0=0, r1=8 * CAP):
        return [((1, e, f), r0, r1) for f in range(lo, hi)]

    def l2(e, lo, hi, r0=0, r1=8 * CAP):
        return [((2, e, n), r0, r1) for n in range(lo, hi)]

    def far(k):
        fwd[k].wait_recv()
        d_s[k].start()

    first = ORDER[0]
    run(l1(first, 0, NF, 0, NEAR), False)
    far(0)
    far(2)
    for n in (0, 2):
        run(l2(first, n, n + 2, 0, NEAR), False)
        send(NEAR_PEERS, 2 * n, 4, first)
    far(1)
    far(3)
    for k in range(CH):
        d_s[k].wait_recv()
    gather(3)
    def whole(e, cuts):
        run(l1(e, 0, NF))
        for lo, hi in cuts:
            run(l2(e, lo, hi))
            send(FAR_PEERS + NEAR_PEERS, 2 * lo, 2 * (hi - lo), e)

    whole(ORDER[1], ((0, 1), (1, 2), (2, 4)))
    run(l1(first, 0, NF, NEAR))
    run(l2(first, 0, N4, NEAR))
    send(FAR_PEERS, 0, N8, first)
    whole(ORDER[2], ((0, 2), (2, 4)))
    last = ORDER[3]
    run(l1(last, 0, 4))
    run(l1(last, 4, NF))
    for lo, hi in ((0, 2), (2, 3), (3, 4)):
        run(l2(last, lo, hi))
        send(NEAR_PEERS + FAR_PEERS, 2 * lo, 2 * (hi - lo), last)

    for n in range(N8):
        for cp in arrive[n]:
            cp.wait_recv()
        total = jnp.zeros((TOK, NB), F32)
        for r in range(4):
            part = jnp.dot(CM[r], R[r, :, :, n].reshape(128, NB), preferred_element_type=F32)
            g0 = GB[r * 2]
            g1 = GB[r * 2 + 1]
            g0 = jnp.concatenate([g0, g0], axis=1)
            g1 = jnp.concatenate([g1, g1], axis=1)
            total = total + (g0 * part[:TOK] + g1 * part[TOK:]).astype(BF16).astype(F32)
        y_ref[:, n * NB:(n + 1) * NB] = total.astype(BF16)

    for cp in metas + own_y + own_x + [own_s] + fwd + y_s + x_s + d_s + sends:
        cp.wait_send()


def solution(mesh):
    row_spec = P(('dp', 'grp', 'ing'))
    exp_spec = P(('grp', 'ing'))

    def local_fn(tokens, expert_ids, gate_vals, w_one, w_three, w_two):
        ids = expert_ids.reshape(TOK, 4).T
        gates = gate_vals.reshape(TOK, 4).T
        dma = pltpu.SemaphoreType.DMA
        anywhere = pl.BlockSpec(memory_space=pl.ANY)
        vmem = pl.BlockSpec(memory_space=pltpu.VMEM)
        return pl.pallas_call(
            kernel,
            out_shape=pltpu.VMEM((TOK, D), BF16),
            in_specs=[anywhere, anywhere, anywhere, anywhere, anywhere, anywhere],
            out_specs=vmem,
            scratch_shapes=[
                pltpu.VMEM((4, TOK), I32), pltpu.VMEM((4, TOK), F32),
                pltpu.VMEM((NS, D, 2 * FC), BF16),
                pltpu.VMEM((4, 2 * TOK, D), BF16),
                pltpu.VMEM((EL, 8 * CAP, D), BF16),
                pltpu.VMEM((2, 8 * CAP, FF), BF16),
                pltpu.VMEM((EL, 8, N8, CAP, NB), BF16),
                pltpu.VMEM((4, 2, EL, N8, CAP, NB), BF16),
                pltpu.VMEM((4, 2 * TOK, TOK), BF16),
                pltpu.VMEM((8, TOK, TOK), F32),
                pltpu.VMEM((4, 128, 256), BF16),
                pltpu.VMEM((8, 8, TOK), F32),
                dma((NS,)), dma((NS,)), dma(()), dma((2,)),
                dma((6, CH)), dma((6, CH)), dma((1,)), dma((1,)),
                dma((7,)), dma((7,)),
                dma((72,)), dma((72,)),
            ],
            compiler_params=pltpu.CompilerParams(collective_id=0, has_side_effects=True, vmem_limit_bytes=65000000),
        )(ids, gates, tokens, w_one, w_three, w_two)

    return jax.shard_map(local_fn, mesh=mesh, in_specs=(row_spec, row_spec, row_spec, exp_spec, exp_spec, exp_spec), out_specs=row_spec, check_vma=False)
```

```python
import functools

import jax
import jax.numpy as jnp
from jax import lax
from jax.experimental import pallas as pl
from jax.experimental.pallas import tpu as pltpu
from jax.sharding import PartitionSpec as P

MESH = pl.DeviceIdType.MESH
BF16 = jnp.bfloat16
F32 = jnp.float32
I32 = jnp.int32

TOK = 128
D = 2048
FF = 1792
EL = 4
CAP = 16
FC = 256
NF = FF // FC
NC = 512
N4 = D // NC
NB = 256
N8 = D // NB
CH = 4
CR = TOK // CH

NS = 23

BLOCK = {(1, 0, 0): 0, (1, 0, 1): 1, (0, 0, 0): 2, (0, 0, 1): 3,
         (0, 1, 0): 4, (0, 1, 1): 5, (1, 1, 0): 6, (1, 1, 1): 7}
NEAR = 6 * CAP
NEAR_PEERS = [(1, 0, 0), (0, 1, 0), (1, 0, 1), (0, 1, 1), (0, 0, 1)]
FAR_PEERS = [(1, 1, 0), (1, 1, 1)]

ORDER = (1, 0, 2, 3)
FETCH = []
for _e in ORDER:
    FETCH += [(1, _e, _f) for _f in range(NF)] + [(2, _e, _n) for _n in range(N4)]


def kernel(ids_hbm, gate_hbm, tok_hbm, w1, w3, w2, y_ref,
           ids_ref, gate_ref, ring, T, X, act, E, R, CM, GB, GH, META,
           ws_a, ws_b, tsem, isem, bs, br, ss, sr, ms, mr, es, er):
    g = lax.axis_index('grp')
    y = lax.axis_index('ing')
    x = g // 2
    c = g % 2

    def peer(dy, dx, dc):
        return {'ing': (y + dy) % 2, 'grp': ((x + dx) % 2) * 2 + (c + dc) % 2}

    def remote(src, dst, s, r, to):
        return pltpu.make_async_remote_copy(src_ref=src, dst_ref=dst, send_sem=s, recv_sem=r, device_id=peer(*to), device_id_type=MESH)

    barrier = pltpu.get_barrier_semaphore()
    direct = [(0, 0, 1), (0, 1, 0), (1, 0, 0), (1, 0, 1)]
    for p in direct:
        pl.semaphore_signal(barrier, inc=1, device_id=peer(*p), device_id_type=MESH)

    def w13(e, f, slot):
        col = pl.ds(pl.multiple_of(f * FC, FC), FC)
        return (pltpu.make_async_copy(w1.at[e, :, col], ring.at[slot, :, pl.ds(0, FC)], ws_a.at[slot]),
                pltpu.make_async_copy(w3.at[e, :, col], ring.at[slot, :, pl.ds(FC, FC)], ws_b.at[slot]))

    def w2c(e, n, slot):
        return (pltpu.make_async_copy(w2.at[e, :, pl.ds(n * NC, NC)], ring.at[slot, pl.ds(0, FF), :], ws_a.at[slot]),)

    def start(copies):
        for cp in copies:
            cp.start(priority=1)

    def wait(copies):
        for cp in copies:
            cp.wait()

    own = pltpu.make_async_copy(tok_hbm, T.at[0, pl.ds(0, TOK), :], tsem)
    small = [pltpu.make_async_copy(ids_hbm, ids_ref, isem.at[0]), pltpu.make_async_copy(gate_hbm, gate_ref, isem.at[1])]
    for cp in small:
        cp.start()
    own.start()
    slot_of = {}
    queue = list(FETCH)

    def fetch(chunk):
        layer, e, j = chunk
        return (w13 if layer == 1 else w2c)(e, j, slot_of[chunk])

    def refill(slot):
        if queue:
            chunk = queue.pop(0)
            slot_of[chunk] = slot
            start(fetch(chunk))

    for cp in small:
        cp.wait()
    META[0] = jnp.concatenate([ids_ref[...].astype(F32), gate_ref[...]], axis=0)
    pl.semaphore_wait(barrier, len(direct))

    metas = [remote(META.at[i], META.at[j], ms.at[k], mr.at[k], to) for k, (i, j, to) in enumerate([
        (0, 4, (1, 0, 0)), (0, 2, (0, 1, 0)), (0, 1, (0, 0, 1)),
        (4, 5, (0, 0, 1)), (4, 6, (0, 1, 0)), (2, 3, (0, 0, 1)), (6, 7, (0, 0, 1))])]
    for m in metas[:3]:
        m.start()
    own.wait()

    def rows(k):
        return pl.ds(k * CR, CR)

    def rows2(k):
        return pl.ds(TOK + k * CR, CR)

    own_y = [remote(T.at[0, rows(k)], T.at[2, rows(k)], bs.at[0, k], br.at[0, k], (1, 0, 0)) for k in range(CH)]
    own_x = [remote(T.at[0, rows(k)], T.at[1, rows(k)], bs.at[1, k], br.at[1, k], (0, 1, 0)) for k in range(CH)]
    own_s = remote(T.at[0, pl.ds(0, TOK)], T.at[0, pl.ds(TOK, TOK)], ss.at[0], sr.at[0], (0, 0, 1))
    fwd = [remote(T.at[2 if k < CH // 2 else 1, rows(k)], T.at[3, rows(k)], bs.at[2, k], br.at[2, k],
                  (0, 1, 0) if k < CH // 2 else (1, 0, 0)) for k in range(CH)]
    y_s = [remote(T.at[2, rows(k)], T.at[2, rows2(k)], bs.at[3, k], br.at[3, k], (0, 0, 1)) for k in range(CH)]
    x_s = [remote(T.at[1, rows(k)], T.at[1, rows2(k)], bs.at[4, k], br.at[4, k], (0, 0, 1)) for k in range(CH)]
    d_s = [remote(T.at[3, rows(k)], T.at[3, rows2(k)], bs.at[5, k], br.at[5, k], (0, 0, 1)) for k in range(CH)]
    own_y[0].start()
    own_x[0].start()
    metas[0].wait_recv()
    metas[4].start()
    metas[3].start()
    metas[1].wait_recv()
    metas[5].start()
    for k in range(1, CH):
        own_y[k].start()
        own_x[k].start()
    own_s.start()

    for i in range(NS):
        refill(i)

    metas[4].wait_recv()
    metas[6].start()
    for i in (2, 3, 5, 6):
        metas[i].wait_recv()
    sub = lax.broadcasted_iota(I32, (TOK, TOK), 0)
    lane = lax.broadcasted_iota(I32, (TOK, TOK), 1)
    base = ((g * 2 + y) * EL).astype(F32)
    hot_rows = []
    for h in range(8):
        ids_h = META[h][0:4, :]
        for e in range(EL):
            hot_rows.append(jnp.sum(jnp.where(ids_h == base + e, 1.0, 0.0), axis=0, keepdims=True))
    hot = jnp.concatenate(hot_rows, axis=0)
    rank = jnp.dot(hot.astype(BF16), (sub < lane).astype(BF16), preferred_element_type=F32)
    key = jnp.where(hot > 0.0, rank, -1.0)
    slot16 = lax.broadcasted_iota(I32, (CAP, TOK), 0).astype(F32)
    zero16 = jnp.zeros((CAP, TOK), F32)
    for q in range(4):
        parts = []
        for e in range(EL):
            for dc in range(2):
                r = (q * 2 + dc) * EL + e
                hit = jnp.where(key[r:r + 1, :] == slot16, 1.0, 0.0)
                parts.append(jnp.concatenate([hit, zero16] if dc == 0 else [zero16, hit], axis=1))
        GH[q] = jnp.concatenate(parts, axis=0).astype(BF16)

    lower = (lane < sub).astype(BF16)
    lane_f = lane.astype(F32)
    meta_t = jnp.transpose(jnp.concatenate([META[0], jnp.zeros((TOK - 8, TOK), F32)], axis=0))
    ids_c = [meta_t[:, k:k + 1] for k in range(4)]
    gate_c = [meta_t[:, 4 + k:5 + k] for k in range(4)]
    hot_t = sum(jnp.where(ids_c[k] == lane_f, 1.0, 0.0) for k in range(4))
    rank_t = jnp.dot(lower, hot_t.astype(BF16), preferred_element_type=F32)
    row_of, grp_of = [], []
    for k in range(4):
        slot = jnp.sum(jnp.where(ids_c[k] == lane_f, rank_t, 0.0), axis=1, keepdims=True).astype(I32)
        idi = ids_c[k].astype(I32)
        row_of.append((((idi >> 2) + y) & 1) * 64 + (idi & 3) * CAP + slot)
        grp_of.append((((idi >> 4) + x) & 1) * 2 + (((idi >> 3) + c) & 1))
    for r in range(4):
        for u in range(2):
            sel = [grp_of[2 * m + u] == r for m in range(2)]
            row = jnp.where(sel[0], row_of[u], jnp.where(sel[1], row_of[2 + u], -1))
            gate = jnp.where(sel[0], gate_c[u], jnp.where(sel[1], gate_c[2 + u], 0.0))
            CM[r, u * TOK:(u + 1) * TOK, :] = jnp.where(row == lane, 1.0, 0.0).astype(BF16)
            GB[r * 2 + u] = jnp.broadcast_to(gate, (TOK, TOK))

    def gather(q):
        dy, dx = q // 2, q % 2
        for n in range(N4):
            cols = pl.ds(n * NC, NC)
            got = jnp.dot(GH[q], T[q, :, cols], preferred_element_type=F32).astype(BF16)
            for e in range(EL):
                for dc in range(2):
                    i = (e * 2 + dc) * CAP
                    X[e, pl.ds(BLOCK[(dy, dx, dc)] * CAP, CAP), cols] = got[i:i + CAP, :]

    def far(k):
        fwd[k].wait_recv()
        d_s[k].start()

    for k in range(CH):
        own_y[k].wait_recv()
        y_s[k].start()
        if k < CH // 2:
            fwd[k].start()
        own_x[k].wait_recv()
        x_s[k].start()
        if k >= CH // 2:
            fwd[k].start()
    own_s.wait_recv()
    gather(0)
    for k in range(CH):
        y_s[k].wait_recv()
        x_s[k].wait_recv()
    gather(1)
    gather(2)

    waited = set()

    def layer1(chunk, r0, r1):
        _, e, f = chunk
        h = jnp.dot(X[e, r0:r1, :], ring[slot_of[chunk]], preferred_element_type=F32)
        h1 = h[:, :FC]
        act[e % 2, r0:r1, f * FC:(f + 1) * FC] = (jax.nn.silu(h1) * h[:, FC:]).astype(BF16)

    def layer2(chunk, r0, r1):
        _, e, n = chunk
        out = jnp.dot(act[e % 2, r0:r1, :], ring[slot_of[chunk], 0:FF, :], preferred_element_type=F32).astype(BF16)
        for t in range(2):
            blk = out[:, t * NB:(t + 1) * NB]
            E[e, r0 // CAP:r1 // CAP, 2 * n + t] = blk.reshape((r1 - r0) // CAP, CAP, NB)
            if r0 == 0:
                R[0, 0, e, 2 * n + t] = blk[32:48, :]

    def run(todo, last=True):
        for chunk, _, _ in todo:
            if chunk not in waited:
                waited.add(chunk)
                wait(fetch(chunk))
        for chunk, r0, r1 in todo:
            (layer1 if chunk[0] == 1 else layer2)(chunk, r0, r1)
        if last:
            for chunk, _, _ in todo:
                refill(slot_of[chunk])

    sends = []
    arrive = [[] for n in range(N8)]

    def send(peers, n0, nn, e):
        for p in peers:
            dy, dx, dc = p
            k = len(sends)
            cp = remote(E.at[e, BLOCK[p], pl.ds(n0, nn)], R.at[dx * 2 + dc, dy, e, pl.ds(n0, nn)], es.at[k], er.at[k], p)
            cp.start()
            sends.append(cp)
            arrive[n0].append(cp)

    def l1(e, lo, hi, r0=0, r1=8 * CAP):
        return [((1, e, f), r0, r1) for f in range(lo, hi)]

    def l2(e, lo, hi, r0=0, r1=8 * CAP):
        return [((2, e, n), r0, r1) for n in range(lo, hi)]

    def far(k):
        fwd[k].wait_recv()
        d_s[k].start()

    first = ORDER[0]
    run(l1(first, 0, NF, 0, NEAR), False)
    far(0)
    far(2)
    for n in (0, 2):
        run(l2(first, n, n + 2, 0, NEAR), False)
        send(NEAR_PEERS, 2 * n, 4, first)
    far(1)
    far(3)
    for k in range(CH):
        d_s[k].wait_recv()
    gather(3)
    def whole(e, cuts):
        run(l1(e, 0, NF))
        for lo, hi in cuts:
            run(l2(e, lo, hi))
            send(FAR_PEERS + NEAR_PEERS, 2 * lo, 2 * (hi - lo), e)

    whole(ORDER[1], ((0, 1), (1, 2), (2, 4)))
    run(l1(first, 0, NF, NEAR))
    run(l2(first, 0, N4, NEAR))
    send(FAR_PEERS, 0, N8, first)
    whole(ORDER[2], ((0, 2), (2, 4)))
    last = ORDER[3]
    run(l1(last, 0, 4))
    run(l1(last, 4, NF))
    for lo, hi in ((0, 2), (2, 3), (3, 4)):
        run(l2(last, lo, hi))
        send(NEAR_PEERS + FAR_PEERS, 2 * lo, 2 * (hi - lo), last)

    for n in range(N8):
        for cp in arrive[n]:
            cp.wait_recv()
        total = jnp.zeros((TOK, NB), F32)
        for r in range(4):
            part = jnp.dot(CM[r], R[r, :, :, n].reshape(128, NB), preferred_element_type=F32)
            g0 = GB[r * 2]
            g1 = GB[r * 2 + 1]
            g0 = jnp.concatenate([g0, g0], axis=1)
            g1 = jnp.concatenate([g1, g1], axis=1)
            total = total + (g0 * part[:TOK] + g1 * part[TOK:]).astype(BF16).astype(F32)
        y_ref[:, n * NB:(n + 1) * NB] = total.astype(BF16)

    for cp in metas + own_y + own_x + [own_s] + fwd + y_s + x_s + d_s + sends:
        cp.wait_send()


def solution(mesh):
    row_spec = P(('dp', 'grp', 'ing'))
    exp_spec = P(('grp', 'ing'))

    def local_fn(tokens, expert_ids, gate_vals, w_one, w_three, w_two):
        ids = expert_ids.reshape(TOK, 4).T
        gates = gate_vals.reshape(TOK, 4).T
        dma = pltpu.SemaphoreType.DMA
        anywhere = pl.BlockSpec(memory_space=pl.ANY)
        vmem = pl.BlockSpec(memory_space=pltpu.VMEM)
        return pl.pallas_call(
            kernel,
            out_shape=pltpu.VMEM((TOK, D), BF16),
            in_specs=[anywhere, anywhere, anywhere, anywhere, anywhere, anywhere],
            out_specs=vmem,
            scratch_shapes=[
                pltpu.VMEM((4, TOK), I32), pltpu.VMEM((4, TOK), F32),
                pltpu.VMEM((NS, D, 2 * FC), BF16),
                pltpu.VMEM((4, 2 * TOK, D), BF16),
                pltpu.VMEM((EL, 8 * CAP, D), BF16),
                pltpu.VMEM((2, 8 * CAP, FF), BF16),
                pltpu.VMEM((EL, 8, N8, CAP, NB), BF16),
                pltpu.VMEM((4, 2, EL, N8, CAP, NB), BF16),
                pltpu.VMEM((4, 2 * TOK, TOK), BF16),
                pltpu.VMEM((8, TOK, TOK), F32),
                pltpu.VMEM((4, 128, 256), BF16),
                pltpu.VMEM((8, 8, TOK), F32),
                dma((NS,)), dma((NS,)), dma(()), dma((2,)),
                dma((6, CH)), dma((6, CH)), dma((1,)), dma((1,)),
                dma((7,)), dma((7,)),
                dma((72,)), dma((72,)),
            ],
            compiler_params=pltpu.CompilerParams(collective_id=0, has_side_effects=True, vmem_limit_bytes=65000000),
        )(ids, gates, tokens, w_one, w_three, w_two)

    return jax.shard_map(local_fn, mesh=mesh, in_specs=(row_spec, row_spec, row_spec, exp_spec, exp_spec, exp_spec), out_specs=row_spec, check_vma=False)
```
